32 devices in a mesh: view: 8 (over z, y), head: 4 (over x, core).
Axes of the slice: x: 2, y: 2, z: 4, core: 2. Of those that a mesh axis runs over, the one named last changes fastest.
Arguments:
- query_rows: bfloat16 [8192, 1024], P('view', 'head'), may hold values from -20 to 20
- key_rows: bfloat16 [8192, 1024], P('view', 'head'), may hold values from -6 to 6
- value_rows: bfloat16 [8192, 1024], P('view', 'head'), may hold values from -12 to 12
- out_weight: bfloat16 [1024, 1024], replicated, may hold values from -0.1875 to 0.1875
- out_grad: bfloat16 [8192, 1024], P('view', 'head'), may hold values from -12 to 12
- source_view: int32 [8, 16], replicated, may hold values from 0 to 7, as said below
- source_block: int32 [8, 16], replicated, may hold values from 0 to 7
Outputs:
- mixed_out: bfloat16 [8192, 1024], P('view', 'head')
- query_grad: bfloat16 [8192, 1024], P('view', 'head')
- key_grad: bfloat16 [8192, 1024], P('view', 'head')
- value_grad: bfloat16 [8192, 1024], P('view', 'head')
The draws below stay inside these ranges and needn't reach their ends.
Inputs may be any that keep to these rules, and one draw needn't show every extreme that they name: `source_view`: for each query view the 16 slots name distinct pairs of source view and block. No source view is named by more than 4 slots of one query view, and for every query view some source view is named by exactly 4 of its slots.
All inputs are finite; a program needn't handle non-finite values.
Results may differ from the reference program's by a relative error of at most 0.014.
Values may be sent and summed in bfloat16 or wider, within the bound.
No kernel may reach another device: no remote copies, remote signals or barrier semaphores. Data moves between devices by JAX's collectives and lax.ppermute only.
A program may use at most 128 MiB of HBM per device.

```python
import jax
import jax.numpy as jnp
from jax import lax

D = 1024
HEADS = 16
HEAD_DIM = 64
BLOCK_TOKENS = 128
SLOTS_PER_QUERY = 16
VIEW_TOK = 1024
TOTAL_VIEWS = 8
KEYS = 2048
CAP = 4


def routing(key):
    block_count = VIEW_TOK // BLOCK_TOKENS
    unit_count = TOTAL_VIEWS * CAP
    unit_source = jnp.arange(unit_count, dtype=jnp.int32) // CAP
    popular = jax.random.randint(jax.random.fold_in(key, 11), (TOTAL_VIEWS,), 0, 4)
    forced = jax.random.randint(jax.random.fold_in(key, 12), (TOTAL_VIEWS,), 0, TOTAL_VIEWS)
    jitter = jax.random.randint(jax.random.fold_in(key, 13), (TOTAL_VIEWS, unit_count), 0, 4096)
    block_ranking = jitter + 2048 * popular[unit_source][None, :] + (1 << 20) * (unit_source[None, :] == forced[:, None]).astype(jnp.int32)
    block_ranking = block_ranking * unit_count + jnp.arange(unit_count, dtype=jnp.int32)[None, :]
    selected_blocks = jnp.argsort(-block_ranking, axis=1)[:, :SLOTS_PER_QUERY].astype(jnp.int32)
    source = selected_blocks // CAP
    copies = selected_blocks % CAP
    shuffle = jax.random.randint(jax.random.fold_in(key, 14), (TOTAL_VIEWS, TOTAL_VIEWS, block_count), 0, 1 << 16)
    shuffle = shuffle * block_count + jnp.arange(block_count, dtype=jnp.int32)[None, None, :]
    perms = jnp.argsort(shuffle, axis=-1).astype(jnp.int32)
    per_view = perms[jnp.arange(TOTAL_VIEWS, dtype=jnp.int32)[:, None], source]
    blocks = jnp.take_along_axis(per_view, copies[:, :, None], axis=2)[:, :, 0]
    return (source.astype(jnp.int32), blocks.astype(jnp.int32))


def draw_source_view(key, part):
    return routing(key)[0]


def draw_source_block(key, part):
    return routing(key)[1]


def draw_query_rows(key, part):
    row_count = TOTAL_VIEWS * VIEW_TOK
    result = 2.0 * jax.random.truncated_normal(jax.random.fold_in(key, 35), -6.0, 6.0, (row_count, D))
    return result.astype(jnp.bfloat16)


def draw_key_rows(key, part):
    row_count = TOTAL_VIEWS * VIEW_TOK
    result = jax.random.truncated_normal(jax.random.fold_in(key, 43), -6.0, 6.0, (row_count, D))
    return result.astype(jnp.bfloat16)


def steps_of(key, dims, shards, least, top_value):
    loudness = 1.0
    for dim, shards_of in shards:
        draws = jax.random.uniform(jax.random.fold_in(jax.random.fold_in(key, 6), dim), (shards_of,), jnp.float32, least / len(shards), top_value / len(shards))
        loudness = loudness * jnp.repeat(jnp.exp(draws), dims[dim] // shards_of).reshape((-1,) + (1,) * (len(dims) - 1 - dim))
    return loudness


def normal_values(rng, extent, spread, most, split=(), kind=jnp.bfloat16):
    loudness = steps_of(rng, extent, split, -0.22, 0.18) if split else 1.0
    entries = jax.random.normal(rng, extent, jnp.float32) * spread * loudness
    return jnp.minimum(jnp.maximum(entries, -most), most).astype(kind)


def setup_inputs(seed: int = 0) -> dict:
    splits = jax.random.split(jax.random.key(seed), 8)
    query_rows = draw_query_rows(jax.random.fold_in(splits[7], 71), 0)
    key_rows = draw_key_rows(jax.random.fold_in(splits[7], 71), 0)
    value_rows = normal_values(splits[2], (TOTAL_VIEWS * VIEW_TOK, D), 2.0, 12.0, ((0, 8), (1, 4)))
    out_weight = normal_values(splits[3], (D, D), D ** -0.5, 0.1875)
    out_grad = normal_values(splits[4], (TOTAL_VIEWS * VIEW_TOK, D), 2.0, 12.0, ((0, 8), (1, 4)))
    source_view = draw_source_view(jax.random.fold_in(splits[7], 71), 0)
    source_block = draw_source_block(jax.random.fold_in(splits[7], 71), 0)
    return dict(query_rows=query_rows, key_rows=key_rows, value_rows=value_rows, out_weight=out_weight, out_grad=out_grad, source_view=source_view, source_block=source_block)


def reference(query_rows, key_rows, value_rows, out_weight, out_grad, source_view, source_block):
    score_scale = HEAD_DIM ** -0.5
    leading_rows = source_view * VIEW_TOK + source_block * BLOCK_TOKENS
    block_passes = jnp.arange(BLOCK_TOKENS, dtype=jnp.int32)
    needed_blocks = (leading_rows[:, :, None] + block_passes[None, None, :]).reshape(TOTAL_VIEWS, SLOTS_PER_QUERY * BLOCK_TOKENS).astype(jnp.int32)
    query_views = query_rows.reshape(TOTAL_VIEWS, VIEW_TOK, D)
    grad_views = out_grad.reshape(TOTAL_VIEWS, VIEW_TOK, D)

    def one_view(totals, inputs):
        grad_keys, grad_values = totals
        query_view, grad_view, index = inputs
        key_heads = jnp.take(key_rows, index, axis=0).reshape(KEYS, HEADS, HEAD_DIM).astype(jnp.float32)
        value_heads = jnp.take(value_rows, index, axis=0).reshape(KEYS, HEADS, HEAD_DIM).astype(jnp.float32)
        query_heads = query_view.reshape(VIEW_TOK, HEADS, HEAD_DIM).astype(jnp.float32)
        scores = jnp.einsum("qhd,khd->hqk", query_heads, key_heads) * score_scale
        row_top = jnp.max(scores, axis=-1, keepdims=True)
        shifted = jnp.exp(scores - row_top)
        probability = shifted / jnp.sum(shifted, axis=-1, keepdims=True)
        weights = lax.optimization_barrier(probability.astype(jnp.bfloat16))
        attended = jnp.einsum("hqk,khd->qhd", weights.astype(jnp.float32), value_heads)
        attended = lax.optimization_barrier(attended.reshape(VIEW_TOK, D).astype(jnp.bfloat16))
        mixed = jnp.dot(attended, out_weight, preferred_element_type=jnp.float32).astype(jnp.bfloat16)
        attended_grad = jnp.dot(grad_view, out_weight.T, preferred_element_type=jnp.float32)
        attended_grad = lax.optimization_barrier(attended_grad.astype(jnp.bfloat16))
        grad_heads = attended_grad.reshape(VIEW_TOK, HEADS, HEAD_DIM).astype(jnp.float32)
        out_heads = attended.reshape(VIEW_TOK, HEADS, HEAD_DIM).astype(jnp.float32)
        grad_prob = jnp.einsum("qhd,khd->hqk", grad_heads, value_heads)
        row_delta = jnp.einsum("qhd,qhd->hq", out_heads, grad_heads)[:, :, None]
        grad_scores = lax.optimization_barrier((probability * (grad_prob - row_delta)).astype(jnp.bfloat16))
        grad_scores = grad_scores.astype(jnp.float32)
        query_grad = jnp.einsum("hqk,khd->qhd", grad_scores, key_heads) * score_scale
        query_grad = query_grad.reshape(VIEW_TOK, D).astype(jnp.bfloat16)
        key_part = (jnp.einsum("hqk,qhd->khd", grad_scores, query_heads) * score_scale).reshape(KEYS, D)
        value_part = jnp.einsum("hqk,qhd->khd", weights.astype(jnp.float32), grad_heads).reshape(KEYS, D)
        grad_keys = grad_keys.at[index].add(key_part)
        grad_values = grad_values.at[index].add(value_part)
        return (grad_keys, grad_values), (mixed, query_grad)

    zero_rows = jnp.zeros((TOTAL_VIEWS * VIEW_TOK, D), jnp.float32)
    (grad_keys, grad_values), (mixed, query_grad) = lax.scan(one_view, (zero_rows, zero_rows), (query_views, grad_views, needed_blocks))
    mixed_out = mixed.reshape(TOTAL_VIEWS * VIEW_TOK, D)
    query_grad = query_grad.reshape(TOTAL_VIEWS * VIEW_TOK, D)
    return mixed_out, query_grad, grad_keys.astype(jnp.bfloat16), grad_values.astype(jnp.bfloat16)
```

```python
import functools

import jax
import jax.numpy as jnp
from jax import lax
from jax.experimental import pallas as pl
from jax.experimental.pallas import tpu as pltpu
from jax.sharding import PartitionSpec as P

HEAD_DIM = 64
BLOCK_TOKENS = 128
LOG2E = 1.4426950408889634
F32 = jnp.float32
BF16 = jnp.bfloat16


def join(a, b):
    return jnp.concatenate([a[:, :HEAD_DIM], b[:, :HEAD_DIM]], axis=1)


def join_high(a, b):
    return jnp.concatenate([a[:, HEAD_DIM:], b[:, HEAD_DIM:]], axis=1)


def dot(a, b):
    return jnp.dot(a, b, preferred_element_type=F32)


def pack_kernel(q_ref, k_ref, v_ref, kv_ref, qp_ref):
    rows = q_ref.shape[0]
    for pair in range(q_ref.shape[1] // 128):
        lanes = slice(128 * pair, 128 * (pair + 1))
        k, v = k_ref[:, lanes], v_ref[:, lanes]
        kv_ref[0, 2 * pair] = join(k, v)
        kv_ref[0, 2 * pair + 1] = join_high(k, v)
        top, low = q_ref[: rows // 2, lanes], q_ref[rows // 2 :, lanes]
        qp_ref[0, 2 * pair] = join(top, low)
        qp_ref[0, 2 * pair + 1] = join_high(top, low)


def pack(q, k, v):
    tokens, columns = q.shape
    half = tokens // 2
    heads = columns // HEAD_DIM
    rows = pl.BlockSpec((half, columns), lambda i: (i, 0))
    return pl.pallas_call(
        pack_kernel,
        grid=(2,),
        in_specs=[rows] * 3,
        out_specs=[
            pl.BlockSpec((1, heads, half, 128), lambda i: (i, 0, 0, 0)),
            pl.BlockSpec((1, heads, half // 2, 128), lambda i: (i, 0, 0, 0)),
        ],
        out_shape=[
            jax.ShapeDtypeStruct((2, heads, half, 128), BF16),
            jax.ShapeDtypeStruct((2, heads, half // 2, 128), BF16),
        ],
        name="pack",
    )(q, k, v)


def unpack_kernel(kv_ref, qp_ref, q_ref, k_ref, v_ref):
    rows = q_ref.shape[0]
    for pair in range(q_ref.shape[1] // 128):
        lanes = slice(128 * pair, 128 * (pair + 1))
        a, b = kv_ref[0, 2 * pair], kv_ref[0, 2 * pair + 1]
        k_ref[:, lanes] = join(a, b)
        v_ref[:, lanes] = join_high(a, b)
        a, b = qp_ref[0, 2 * pair], qp_ref[0, 2 * pair + 1]
        q_ref[: rows // 2, lanes] = join(a, b)
        q_ref[rows // 2 :, lanes] = join_high(a, b)


def unpack(kv, qp):
    _, heads, half, _ = kv.shape
    columns = heads * HEAD_DIM
    rows = pl.BlockSpec((half, columns), lambda i: (i, 0))
    return pl.pallas_call(
        unpack_kernel,
        grid=(2,),
        in_specs=[
            pl.BlockSpec((1, heads, half, 128), lambda i: (i, 0, 0, 0)),
            pl.BlockSpec((1, heads, half // 2, 128), lambda i: (i, 0, 0, 0)),
        ],
        out_specs=[rows] * 3,
        out_shape=[jax.ShapeDtypeStruct((2 * half, columns), BF16)] * 3,
        name="unpack",
    )(kv, qp)


def grad_kernel(x_ref, og_ref, w_ref, out_ref):
    parts, rows, columns = og_ref.shape
    total = None
    for part in range(parts):
        piece = lax.dot_general(
            og_ref[part],
            w_ref[:, columns * part : columns * (part + 1)],
            (((1,), (1,)), ((), ())),
            preferred_element_type=F32,
        )
        total = piece if total is None else total + piece
    total = total.astype(BF16)
    for pair in range(total.shape[1] // 128):
        lanes = slice(128 * pair, 128 * (pair + 1))
        top, low = total[: rows // 2, lanes], total[rows // 2 :, lanes]
        out_ref[2 * pair] = join(top, low)
        out_ref[2 * pair + 1] = join_high(top, low)


def attended_grads(plane, og, weight, plane_columns):
    parts, rows, columns = og.shape
    depth = parts * columns
    return pl.pallas_call(
        grad_kernel,
        grid_spec=pltpu.PrefetchScalarGridSpec(
            num_scalar_prefetch=1,
            grid=(1,),
            in_specs=[
                pl.BlockSpec((parts, rows, columns), lambda i, x: (0, 0, 0)),
                pl.BlockSpec((plane_columns, depth), lambda i, x: (x[0], 0)),
            ],
            out_specs=pl.BlockSpec(
                (plane_columns // HEAD_DIM, rows // 2, 128), lambda i, x: (0, 0, 0)
            ),
        ),
        out_shape=jax.ShapeDtypeStruct((plane_columns // HEAD_DIM, rows // 2, 128), BF16),
        name="attended_grads",
    )(plane, og, weight)


def mix_kernel(x_ref, own_ref, other_ref, w_ref, out_ref):
    heads, rows, _ = own_ref.shape
    depth = heads * HEAD_DIM
    x = x_ref[0]

    def rows_of(ref):
        top, low = [], []
        for pair in range(heads // 2):
            a, b = ref[2 * pair], ref[2 * pair + 1]
            top.append(join(a, b))
            low.append(join_high(a, b))
        return jnp.concatenate(
            [jnp.concatenate(top, axis=1), jnp.concatenate(low, axis=1)], axis=0
        )

    own = dot(rows_of(own_ref), w_ref[pl.ds(pl.multiple_of(x * depth, depth), depth), :])
    other = dot(
        rows_of(other_ref), w_ref[pl.ds(pl.multiple_of((1 - x) * depth, depth), depth), :]
    )
    mixed = (own + other).astype(BF16)
    width = mixed.shape[1] // 2
    out_ref[0] = mixed[:, :width]
    out_ref[1] = mixed[:, width:]


def mix(plane, own, other, weight):
    heads, rows, _ = own.shape
    width = heads * HEAD_DIM
    whole = pl.BlockSpec((heads, rows, 128), lambda i, x: (0, 0, 0))
    return pl.pallas_call(
        mix_kernel,
        grid_spec=pltpu.PrefetchScalarGridSpec(
            num_scalar_prefetch=1,
            grid=(1,),
            in_specs=[
                whole,
                whole,
                pl.BlockSpec((weight.shape[0], width), lambda i, x: (0, x[0])),
            ],
            out_specs=pl.BlockSpec((2, 2 * rows, width // 2), lambda i, x: (0, 0, 0)),
        ),
        out_shape=jax.ShapeDtypeStruct((2, 2 * rows, width // 2), BF16),
        name="mix",
    )(plane, own, other, weight)


def bring_sources(c_ref, own_ref, other_ref, kv_scr, sem):
    c = c_ref[0]
    first = pltpu.make_async_copy(own_ref, kv_scr.at[c], sem.at[0])
    second = pltpu.make_async_copy(other_ref, kv_scr.at[1 - c], sem.at[1])
    first.start()
    second.start()
    first.wait()
    second.wait()


def place(sv_ref, sb_ref, view, slot, per_half):
    block = sb_ref[view, slot]
    start = pl.multiple_of(lax.rem(block, per_half) * BLOCK_TOKENS, BLOCK_TOKENS)
    return lax.div(block, per_half), sv_ref[view, slot], pl.ds(start, BLOCK_TOKENS)


def gather_slots(sv_ref, sb_ref, view, kv_scr, kvg, kvt):
    per_half = kv_scr.shape[2] // BLOCK_TOKENS
    for slot in range(sv_ref.shape[1]):
        half, source, rows = place(sv_ref, sb_ref, view, slot, per_half)
        block = kv_scr[half, source, rows, :]
        kvg[slot * BLOCK_TOKENS : (slot + 1) * BLOCK_TOKENS, :] = block
        kvt[:, slot * BLOCK_TOKENS : (slot + 1) * BLOCK_TOKENS] = block.T


def turned(block):
    t = block.T
    return jnp.concatenate([t[:HEAD_DIM], t[HEAD_DIM:]], axis=1)


def turned_back(t):
    width = t.shape[1] // 2
    return jnp.concatenate([t[:, :width], t[:, width:]], axis=0).T


def forward_kernel(
    sv_ref, sb_ref, c_ref, own_ref, other_ref, q_ref, e_ref, o_ref, l_ref, kv_scr, kvg, kvt, s_scr, sem
):
    view = pl.program_id(0)

    @pl.when(view == 0)
    def _():
        bring_sources(c_ref, own_ref, other_ref, kv_scr, sem)

    gather_slots(sv_ref, sb_ref, view, kv_scr, kvg, kvt)
    keys, queries = s_scr.shape
    step = 256
    q = turned(q_ref[0]) * jnp.asarray(HEAD_DIM**-0.5, BF16)
    q = jnp.concatenate([q, jnp.zeros_like(q)], axis=0)
    top = None
    for i in range(keys // step):
        s = dot(kvg[i * step : (i + 1) * step, :], q)
        s_scr[i * step : (i + 1) * step, :] = s
        t = jnp.max(s.reshape(step // 8, 8, queries), axis=0)
        top = t if top is None else jnp.maximum(top, t)
    top = jnp.max(top, axis=0, keepdims=True)
    total = None
    for i in range(keys // step):
        e = jnp.exp2((s_scr[i * step : (i + 1) * step, :] - top) * LOG2E)
        t = jnp.sum(e.reshape(step // 8, 8, queries), axis=0)
        total = t if total is None else total + t
        e_ref[0, i * step : (i + 1) * step, :] = e.astype(BF16)
    total = jnp.sum(total, axis=0, keepdims=True)
    l_ref[0] = total
    out = dot(kvt[...], e_ref[0])[HEAD_DIM:] / total
    o_ref[0] = turned_back(out).astype(BF16)


def backward_kernel(
    sv_ref, sb_ref, c_ref, own_ref, other_ref, q_ref, e_ref, o_ref, l_ref, g_ref,
    dq_ref, near_ref, far_ref, kv_scr, kvg, kvt, ds_scr, acc, sem,
):
    view = pl.program_id(0)

    @pl.when(view == 0)
    def _():
        bring_sources(c_ref, own_ref, other_ref, kv_scr, sem)
        acc[...] = jnp.zeros_like(acc)

    gather_slots(sv_ref, sb_ref, view, kv_scr, kvg, kvt)
    keys, queries = ds_scr.shape
    per_half = kv_scr.shape[2] // BLOCK_TOKENS
    step = 256
    q = turned(q_ref[0]) * jnp.asarray(HEAD_DIM**-0.5, BF16)
    q_rows = jnp.concatenate([q, jnp.zeros_like(q)], axis=0).T
    g = (turned(g_ref[0]).astype(F32) / l_ref[0]).astype(BF16)
    delta = jnp.sum(turned(o_ref[0]).astype(F32) * g.astype(F32), axis=0, keepdims=True)
    g = jnp.concatenate([jnp.zeros_like(g), g], axis=0)
    g_rows = g.T
    for i in range(keys // step):
        rows = slice(i * step, (i + 1) * step)
        e = e_ref[0, rows, :]
        dp = dot(kvg[rows, :], g)
        ds = (e.astype(F32) * (dp - delta)).astype(BF16)
        ds_scr[rows, :] = ds
        dkv = dot(ds, q_rows) + dot(e, g_rows)
        for part in range(step // BLOCK_TOKENS):
            slot = i * (step // BLOCK_TOKENS) + part
            half, source, where = place(sv_ref, sb_ref, view, slot, per_half)
            acc[half, source, where, :] += dkv[part * BLOCK_TOKENS : (part + 1) * BLOCK_TOKENS]
    dq = dot(kvt[...], ds_scr[...])[:HEAD_DIM] * (HEAD_DIM**-0.5)
    dq_ref[0] = turned_back(dq).astype(BF16)

    @pl.when(view == pl.num_programs(0) - 1)
    def _():
        c = c_ref[0]
        near_ref[...] = acc[c]
        far_ref[...] = acc[1 - c].astype(BF16)


def attention_specs(views, half):
    hbm = pl.BlockSpec(memory_space=pl.ANY)
    packed = pl.BlockSpec((1, half // 2, 128), lambda i, *_: (i, 0, 0))
    return hbm, packed


def forward(routes, own, other, q, keys):
    views, half, _ = own.shape
    hbm, packed = attention_specs(views, half)
    return pl.pallas_call(
        forward_kernel,
        grid_spec=pltpu.PrefetchScalarGridSpec(
            num_scalar_prefetch=3,
            grid=(views,),
            in_specs=[hbm, hbm, packed],
            out_specs=[
                pl.BlockSpec((1, keys, half), lambda i, *_: (i, 0, 0)),
                packed,
                pl.BlockSpec((1, 1, half), lambda i, *_: (i, 0, 0)),
            ],
            scratch_shapes=[
                pltpu.VMEM((2, views, half, 128), BF16),
                pltpu.VMEM((keys, 128), BF16),
                pltpu.VMEM((128, keys), BF16),
                pltpu.VMEM((keys, half), F32),
                pltpu.SemaphoreType.DMA((2,)),
            ],
        ),
        out_shape=[
            jax.ShapeDtypeStruct((views, keys, half), BF16),
            jax.ShapeDtypeStruct((views, half // 2, 128), BF16),
            jax.ShapeDtypeStruct((views, 1, half), F32),
        ],
        compiler_params=pltpu.CompilerParams(dimension_semantics=("arbitrary",)),
        cost_estimate=pl.CostEstimate(
            flops=views * keys * half * 256 * 2,
            transcendentals=views * keys * half,
            bytes_accessed=views * keys * half * 2,
        ),
        name="forward",
    )(*routes, own, other, q)


def backward(routes, own, other, q, e, o, l, g):
    views, half, _ = own.shape
    keys = e.shape[1]
    hbm, packed = attention_specs(views, half)
    whole = pl.BlockSpec((views, half, 128), lambda i, *_: (0, 0, 0))
    return pl.pallas_call(
        backward_kernel,
        grid_spec=pltpu.PrefetchScalarGridSpec(
            num_scalar_prefetch=3,
            grid=(views,),
            in_specs=[
                hbm,
                hbm,
                packed,
                pl.BlockSpec((1, keys, half), lambda i, *_: (i, 0, 0)),
                packed,
                pl.BlockSpec((1, 1, half), lambda i, *_: (i, 0, 0)),
                packed,
            ],
            out_specs=[packed, whole, whole],
            scratch_shapes=[
                pltpu.VMEM((2, views, half, 128), BF16),
                pltpu.VMEM((keys, 128), BF16),
                pltpu.VMEM((128, keys), BF16),
                pltpu.VMEM((keys, half), BF16),
                pltpu.VMEM((2, views, half, 128), F32),
                pltpu.SemaphoreType.DMA((2,)),
            ],
        ),
        out_shape=[
            jax.ShapeDtypeStruct((views, half // 2, 128), BF16),
            jax.ShapeDtypeStruct((views, half, 128), F32),
            jax.ShapeDtypeStruct((views, half, 128), BF16),
        ],
        compiler_params=pltpu.CompilerParams(dimension_semantics=("arbitrary",)),
        cost_estimate=pl.CostEstimate(
            flops=views * keys * half * 512 * 2,
            transcendentals=0,
            bytes_accessed=views * keys * half * 2,
        ),
        name="backward",
    )(*routes, own, other, q, e, o, l, g)


def plane_body(query_rows, key_rows, value_rows, out_weight, out_grad, source_view, source_block):
    tokens, columns = query_rows.shape
    half = tokens // 2
    heads = columns // HEAD_DIM
    keys = source_view.shape[1] * BLOCK_TOKENS
    group = lax.axis_size("head")
    head_index = lax.axis_index("head")
    core = lax.rem(head_index, 2).astype(jnp.int32).reshape(1)
    plane = lax.div(head_index, 2).astype(jnp.int32).reshape(1)
    partner = [(i, i ^ 1) for i in range(group)]
    across = [(i, i ^ 2) for i in range(group)]
    pairs = [[2 * i, 2 * i + 1] for i in range(group // 2)]

    def core_swap(x):
        return lax.all_to_all(
            x, "head", split_axis=0, concat_axis=0, axis_index_groups=pairs, tiled=True
        )

    def view_swap(x):
        return lax.all_to_all(x, "view", split_axis=0, concat_axis=0, tiled=True)

    kv, qp = pack(query_rows, key_rows, value_rows)
    kv = view_swap(core_swap(kv.reshape(2 * heads, half, 128)))
    qp = view_swap(core_swap(qp.reshape(2 * heads, half // 2, 128)))
    og = out_grad.reshape(1, 2, half, columns)
    og = jnp.broadcast_to(og, (group // 2, 2, half, columns)).reshape(group, half, columns)
    og = lax.all_to_all(og, "head", split_axis=0, concat_axis=0, tiled=True)
    g = view_swap(attended_grads(plane, og, out_weight, 2 * columns))
    kv_other = lax.ppermute(kv, "head", partner)
    routes = (source_view, source_block, core)
    e, o, l = forward(routes, kv, kv_other, qp, keys)
    dq, near, far = backward(routes, kv, kv_other, qp, e, o, l, g)
    o = view_swap(o)
    mixed = mix(plane, o, lax.ppermute(o, "head", across), out_weight)
    mixed_out = core_swap(mixed).reshape(tokens, columns)
    far = lax.ppermute(far, "head", partner)
    dkv = (near + far.astype(F32)).astype(BF16)
    dkv = core_swap(view_swap(dkv))
    dq = core_swap(view_swap(dq))
    grads = unpack(dkv.reshape(2, heads, half, 128), dq.reshape(2, heads, half // 2, 128))
    return (mixed_out, *grads)


def score_rows(query_part, key_heads, score_scale):
    return (
        jnp.einsum("qhd,khd->hqk", query_part, key_heads, preferred_element_type=jnp.float32)
        * score_scale
    )


def body(query_rows, key_rows, value_rows, out_weight, out_grad, source_view, source_block):
    tokens = query_rows.shape[0]
    columns = query_rows.shape[1]
    heads_here = columns // HEAD_DIM
    slot_count = source_view.shape[1]
    key_count = slot_count * BLOCK_TOKENS
    peer_count = lax.axis_size("view")
    capacity = max(1, 2 * slot_count // peer_count)
    block_count = tokens // BLOCK_TOKENS
    view_index = lax.axis_index("view")
    head_index = lax.axis_index("head")
    score_scale = HEAD_DIM ** (-0.5)
    slot_order = jnp.arange(slot_count, dtype=jnp.int32)
    same_view = source_view[:, :, None] == source_view[:, None, :]
    earlier = slot_order[None, :] < slot_order[:, None]
    slot_rank = jnp.sum((same_view & earlier[None]).astype(jnp.int32), axis=2)
    copy_order = jnp.arange(capacity, dtype=jnp.int32)
    matched = (source_view == view_index)[:, :, None] & (
        slot_rank[:, :, None] == copy_order[None, None, :]
    )
    filled = jnp.any(matched, axis=1)
    chosen = jnp.sum(jnp.where(matched, source_block[:, :, None], 0), axis=1)
    own_view = lax.dynamic_index_in_dim(source_view, view_index, 0, keepdims=False)
    own_rank = lax.dynamic_index_in_dim(slot_rank, view_index, 0, keepdims=False)
    landing = own_view * capacity + own_rank
    joined = jnp.concatenate([key_rows, value_rows], axis=1)
    outgoing = jnp.take(
        joined.reshape(block_count, BLOCK_TOKENS, 2 * columns), chosen.reshape(-1), axis=0
    )
    outgoing = outgoing.reshape(peer_count, capacity, BLOCK_TOKENS, 2 * columns)
    incoming = lax.all_to_all(outgoing, "view", split_axis=0, concat_axis=0, tiled=True)
    fetched = jnp.take(
        incoming.reshape(peer_count * capacity, BLOCK_TOKENS, 2 * columns), landing, axis=0
    )
    fetched = fetched.reshape(key_count, 2 * columns)
    query_block = min(512, tokens)
    block_total = tokens // query_block
    key_heads = fetched[:, :columns].reshape(key_count, heads_here, HEAD_DIM)
    value_heads = fetched[:, columns:].reshape(key_count, heads_here, HEAD_DIM)
    query_heads = query_rows.reshape(block_total, query_block, heads_here, HEAD_DIM)

    def forward_step(query_part):
        scores = score_rows(query_part, key_heads, score_scale)
        row_top = jnp.max(scores, axis=-1, keepdims=True)
        shifted = jnp.exp(scores - row_top)
        row_total = jnp.sum(shifted, axis=-1, keepdims=True)
        weights = (shifted / row_total).astype(jnp.bfloat16)
        out_part = jnp.einsum(
            "hqk,khd->qhd", weights, value_heads, preferred_element_type=jnp.float32
        )
        return (out_part.astype(jnp.bfloat16), row_top, row_total)

    attended, row_tops, row_totals = lax.map(forward_step, query_heads)
    attended_rows = attended.reshape(tokens, columns)
    own_rows = lax.dynamic_slice_in_dim(out_weight, head_index * columns, columns, 0)
    part_weight = own_rows
    summed_rows = lax.psum_scatter(
        lax.dot_general(
            part_weight, attended_rows, (((0,), (1,)), ((), ())), preferred_element_type=jnp.float32
        ).astype(jnp.bfloat16),
        "head",
        scatter_dimension=0,
        tiled=True,
    ).astype(jnp.float32)
    mixed_out = summed_rows.T.astype(jnp.bfloat16)
    part_weight = own_rows
    attended_grad = lax.dot_general(
        lax.all_gather(out_grad, "head", axis=1, tiled=True),
        part_weight,
        (((1,), (1,)), ((), ())),
        preferred_element_type=jnp.float32,
    )
    grad_heads = attended_grad.astype(jnp.bfloat16).reshape(
        block_total, query_block, heads_here, HEAD_DIM
    )

    def backward_step(totals, inputs):
        key_total, value_total = totals
        query_part, out_part, grad_part, row_top, row_total = inputs
        scores = score_rows(query_part, key_heads, score_scale)
        probability = jnp.exp(scores - row_top) / row_total
        weights = probability.astype(jnp.bfloat16)
        grad_prob = jnp.einsum(
            "qhd,khd->hqk", grad_part, value_heads, preferred_element_type=jnp.float32
        )
        row_delta = jnp.einsum(
            "qhd,qhd->hq", out_part, grad_part, preferred_element_type=jnp.float32
        )[:, :, None]
        grad_scores = (probability * (grad_prob - row_delta)).astype(jnp.bfloat16)
        query_part_grad = (
            jnp.einsum("hqk,khd->qhd", grad_scores, key_heads, preferred_element_type=jnp.float32)
            * score_scale
        )
        key_total = (
            key_total
            + jnp.einsum(
                "hqk,qhd->khd", grad_scores, query_part, preferred_element_type=jnp.float32
            )
            * score_scale
        )
        value_total = value_total + jnp.einsum(
            "hqk,qhd->khd", weights, grad_part, preferred_element_type=jnp.float32
        )
        return ((key_total, value_total), query_part_grad.astype(jnp.bfloat16))

    zero_keys = jnp.zeros((key_count, heads_here, HEAD_DIM), jnp.float32)
    (key_total, value_total), query_grads = lax.scan(
        backward_step,
        (zero_keys, zero_keys),
        (query_heads, attended, grad_heads, row_tops, row_totals),
    )
    query_grad = query_grads.reshape(tokens, columns)
    slot_grads = jnp.concatenate(
        [key_total.reshape(key_count, columns), value_total.reshape(key_count, columns)], axis=1
    )
    slot_grads = slot_grads.reshape(slot_count, BLOCK_TOKENS * 2 * columns)
    placing = (
        landing[None, :] == jnp.arange(peer_count * capacity, dtype=jnp.int32)[:, None]
    ).astype(jnp.float32)
    outgoing_grads = jnp.dot(placing, slot_grads, precision=lax.Precision.HIGHEST).reshape(
        peer_count, capacity, BLOCK_TOKENS, 2 * columns
    )
    returned = lax.all_to_all(
        outgoing_grads.astype(jnp.bfloat16), "view", split_axis=0, concat_axis=0, tiled=True
    ).astype(outgoing_grads.dtype)
    gathering = (
        chosen.reshape(-1)[None, :] == jnp.arange(block_count, dtype=jnp.int32)[:, None]
    ) & filled.reshape(-1)[None, :]
    summed = jnp.dot(
        gathering.astype(jnp.float32),
        returned.reshape(peer_count * capacity, BLOCK_TOKENS * 2 * columns),
        precision=lax.Precision.HIGHEST,
    )
    summed = summed.reshape(tokens, 2 * columns)
    key_grad = summed[:, :columns].astype(jnp.bfloat16)
    value_grad = summed[:, columns:].astype(jnp.bfloat16)
    return (mixed_out, query_grad, key_grad, value_grad)


def solution(mesh):
    placed = (
        P("view", "head"),
        P("view", "head"),
        P("view", "head"),
        P(),
        P("view", "head"),
        P(),
        P(),
    )
    views, group = mesh.shape["view"], mesh.shape["head"]

    def chosen(*args):
        columns = args[0].shape[1]
        fits = (
            group == 4
            and 2 * columns == views * HEAD_DIM
            and columns % 128 == 0
            and args[0].shape[0] % (4 * BLOCK_TOKENS) == 0
        )
        return plane_body(*args) if fits else body(*args)

    return jax.shard_map(
        chosen,
        mesh=mesh,
        in_specs=placed,
        out_specs=(P("view", "head"), P("view", "head"), P("view", "head"), P("view", "head")),
        check_vma=False,
    )
```

```python
import jax
import jax.numpy as jnp
from jax import lax
from jax.experimental import pallas as pl
from jax.experimental.pallas import tpu as pltpu
from jax.sharding import PartitionSpec as P


HEAD_DIM = 64
BLOCK_TOKENS = 128
LOG2E = 1.4426950408889634
F32 = jnp.float32
BF16 = jnp.bfloat16
HBM = pl.BlockSpec(memory_space=pl.ANY)


def join(a, b):
    return jnp.concatenate([a[:, :HEAD_DIM], b[:, :HEAD_DIM]], axis=1)


def join_high(a, b):
    return jnp.concatenate([a[:, HEAD_DIM:], b[:, HEAD_DIM:]], axis=1)


def dot(a, b):
    return jnp.dot(a, b, preferred_element_type=F32)


def aligned(index, size):
    return pl.ds(pl.multiple_of(index * size, size), size)


def call(kernel, scalars, args, in_specs, out_specs, out_shape, grid=(1,), scratch=(), flops=0):
    return pl.pallas_call(
        kernel,
        grid_spec=pltpu.PrefetchScalarGridSpec(
            num_scalar_prefetch=len(scalars),
            grid=grid,
            in_specs=in_specs,
            out_specs=out_specs,
            scratch_shapes=list(scratch),
        ),
        out_shape=out_shape,
        compiler_params=pltpu.CompilerParams(dimension_semantics=("arbitrary",) * len(grid)),
        cost_estimate=pl.CostEstimate(flops=flops, transcendentals=0, bytes_accessed=0)
        if flops
        else None,
    )(*scalars, *args)


def whole(*shape):
    return pl.BlockSpec(shape, lambda *_: (0,) * len(shape))


def shape_of(*shape, dtype=BF16):
    return jax.ShapeDtypeStruct(shape, dtype)


def messages(count):
    return [(j, i) for j in range(count) for i in range(2)]


def source_of(meta_ref, core, j, i, count):
    return (core ^ i) * count + (meta_ref[1] ^ j)


def pick(meta_ref, ref, j, i, rows):
    head, half = meta_ref[1] ^ j, meta_ref[2] ^ i
    return ref[aligned(half, rows), aligned(head // 2, 128)], head % 2 == 1


def pack_kq(meta_ref, q_ref, k_ref, *outs):
    rows = q_ref.shape[0] // 2
    for out, (j, i) in zip(outs, messages(len(outs) // 2)):
        k, odd = pick(meta_ref, k_ref, j, i, rows)
        q, _ = pick(meta_ref, q_ref, j, i, rows)
        out[...] = jnp.where(odd, join_high(k, q), join(k, q))


def pack_v(meta_ref, v_ref, keep_ref, give_ref):
    rows = v_ref.shape[0] // 2
    for out_ref, half in ((keep_ref, meta_ref[0]), (give_ref, 1 - meta_ref[0])):
        for pair in range(out_ref.shape[0] // 2):
            v = v_ref[aligned(half, rows), 128 * pair : 128 * (pair + 1)]
            top, low = v[: rows // 2], v[rows // 2 :]
            out_ref[2 * pair] = join(top, low)
            out_ref[2 * pair + 1] = join_high(top, low)


def unpack_kq(meta_ref, *refs):
    count = (len(refs) - 4) // 2
    parts, (q_ref, k_ref, scr, sem) = refs[: 2 * count], refs[2 * count :]
    copies = [
        pltpu.make_async_copy(part, scr.at[meta_ref[2] ^ i, meta_ref[1] ^ j], sem.at[n])
        for n, (part, (j, i)) in enumerate(zip(parts, messages(count)))
    ]
    for copy in copies:
        copy.start()
    for copy in copies:
        copy.wait()
    rows = scr.shape[2]
    for half in range(2):
        for pair in range(count // 2):
            lanes = slice(128 * pair, 128 * (pair + 1))
            a, b = scr[half, 2 * pair], scr[half, 2 * pair + 1]
            k_ref[half * rows : (half + 1) * rows, lanes] = join(a, b)
            q_ref[half * rows : (half + 1) * rows, lanes] = join_high(a, b)


def unpack_v(meta_ref, all_ref, got_ref, v_ref, scr, sem):
    c = meta_ref[0]
    count = scr.shape[1]
    copies = [
        pltpu.make_async_copy(
            all_ref.at[pl.ds(c * count, count), pl.ds(0, scr.shape[2])], scr.at[c], sem.at[0]
        ),
        pltpu.make_async_copy(got_ref, scr.at[1 - c], sem.at[1]),
    ]
    for copy in copies:
        copy.start()
    for copy in copies:
        copy.wait()
    rows = 2 * scr.shape[2]
    for half in range(2):
        for pair in range(count // 2):
            lanes = slice(128 * pair, 128 * (pair + 1))
            a, b = scr[half, 2 * pair], scr[half, 2 * pair + 1]
            v_ref[half * rows : half * rows + rows // 2, lanes] = join(a, b)
            v_ref[half * rows + rows // 2 : (half + 1) * rows, lanes] = join_high(a, b)


def attended_grads(place_ref, *refs):
    parts, (keep_ref, got_ref, w_ref, out_ref) = refs[:-4], refs[-4:]
    rows, columns = parts[0].shape
    total = None
    for n, part in enumerate(parts):
        piece = lax.dot_general(
            part[...],
            w_ref[:, aligned(place_ref[1] ^ n, columns)],
            (((1,), (1,)), ((), ())),
            preferred_element_type=F32,
        )
        total = piece if total is None else total + piece
    total = total.astype(BF16)
    for pair in range(total.shape[1] // 128):
        lanes = slice(128 * pair, 128 * (pair + 1))
        top, low = total[: rows // 2, lanes], total[rows // 2 :, lanes]
        out_ref[2 * pair, rows // 2 :, :] = join(top, low)
        out_ref[2 * pair + 1, rows // 2 :, :] = join_high(top, low)
    count = keep_ref.shape[0]
    core = place_ref[1] % 2
    out_ref[pl.ds(core * count, count), : rows // 2, :] = keep_ref[...]
    out_ref[pl.ds((1 - core) * count, count), : rows // 2, :] = got_ref[...]


def combine_v(near_ref, far_ref, o_ref, out_ref):
    rows = near_ref.shape[1]
    out_ref[:, :rows, :] = (near_ref[...] + far_ref[...].astype(F32)).astype(BF16)
    out_ref[:, rows:, :] = o_ref[...]


def mix(place_ref, own_ref, other_ref, w_ref, keep_ref, send_ref):
    heads = own_ref.shape[0]
    depth = heads * HEAD_DIM
    x = place_ref[0]

    def rows_of(ref):
        top, low = [], []
        for pair in range(heads // 2):
            a, b = ref[2 * pair], ref[2 * pair + 1]
            top.append(join(a, b))
            low.append(join_high(a, b))
        return jnp.concatenate(
            [jnp.concatenate(top, axis=1), jnp.concatenate(low, axis=1)], axis=0
        )

    own = dot(rows_of(own_ref), w_ref[aligned(x, depth), :])
    other = dot(rows_of(other_ref), w_ref[aligned(1 - x, depth), :])
    mixed = (own + other).astype(BF16)
    width = mixed.shape[1] // 2
    first = place_ref[1] % 2 == 0
    keep_ref[...] = jnp.where(first, mixed[:, :width], mixed[:, width:])
    send_ref[...] = jnp.where(first, mixed[:, width:], mixed[:, :width])


def place(sv_ref, sb_ref, view, slot, per_part):
    block = sb_ref[view, slot]
    return lax.div(block, per_part), sv_ref[view, slot], aligned(lax.rem(block, per_part), BLOCK_TOKENS)


def gather(sv_ref, sb_ref, view, src, rows_scr, turned_scr):
    per_half = src.shape[2] // BLOCK_TOKENS
    for slot in range(sv_ref.shape[1]):
        half, source, rows = place(sv_ref, sb_ref, view, slot, per_half)
        block = src[half, source, rows, :]
        span = slice(slot * BLOCK_TOKENS, (slot + 1) * BLOCK_TOKENS)
        if rows_scr is not None:
            rows_scr[span, :] = block
        if turned_scr is not None:
            turned_scr[:, span] = block.T


def scatter_folded(sv_ref, sb_ref, view, acc, lhs_ref, rhs_scr):
    per_quarter = acc.shape[2] // BLOCK_TOKENS
    for slot in range(sv_ref.shape[1]):
        quarter, source, rows = place(sv_ref, sb_ref, view, slot, per_quarter)
        span = slice(slot * BLOCK_TOKENS, (slot + 1) * BLOCK_TOKENS)
        acc[lax.div(quarter, 2), source, rows, :] += dot(
            lhs_ref[span, :], rhs_scr[lax.rem(quarter, 2)]
        )


def hand_back(meta_ref, acc, near_ref, far_ref):
    c = meta_ref[0]
    count = acc.shape[1] // 2
    for n, (j, i) in enumerate(messages(count)):
        near_ref[n] = acc[c, source_of(meta_ref, c, j, i, count)]
        far_ref[n] = acc[1 - c, source_of(meta_ref, 1 - c, j, i, count)].astype(BF16)


def hand_back_views(meta_ref, acc, near_ref, far_ref):
    near_ref[...] = acc[meta_ref[0]]
    far_ref[...] = acc[1 - meta_ref[0]].astype(BF16)


def bring(meta_ref, own, other, scr, sem):
    c = meta_ref[0]
    count = len(own) // 2
    copies = []
    for n, (j, i) in enumerate(messages(count)):
        for core, part, s in ((c, own[n], 2 * n), (1 - c, other[n], 2 * n + 1)):
            where = scr.at[core, source_of(meta_ref, core, j, i, count)]
            copies.append(pltpu.make_async_copy(part, where, sem.at[s]))
    for copy in copies:
        copy.start()
    for copy in copies:
        copy.wait()


def unfold(block):
    t = block.T
    return jnp.concatenate([t[:HEAD_DIM], t[HEAD_DIM:]], axis=1)


def fold(t):
    width = t.shape[1] // 2
    return jnp.concatenate([t[:, :width], t[:, width:]], axis=0).T


SCALE = HEAD_DIM**-0.5


def scores(sv_ref, sb_ref, meta_ref, *refs):
    views = (len(refs) - 6) // 2
    own, other = refs[:views], refs[views : 2 * views]
    kq_ref, e_ref, l_ref, rows_scr, s_scr, sem = refs[2 * views :]
    view = pl.program_id(0)

    @pl.when(view == 0)
    def _():
        bring(meta_ref, own, other, kq_ref, sem)

    gather(sv_ref, sb_ref, view, kq_ref, rows_scr, None)
    keys, queries = s_scr.shape
    step = 256
    q = kq_ref[meta_ref[0], view].T[HEAD_DIM:] * jnp.asarray(SCALE, BF16)
    q = jnp.concatenate([q, jnp.zeros_like(q)], axis=0)
    top = None
    for i in range(keys // step):
        s = dot(rows_scr[i * step : (i + 1) * step, :], q)
        s_scr[i * step : (i + 1) * step, :] = s
        t = jnp.max(s.reshape(step // 8, 8, queries), axis=0)
        top = t if top is None else jnp.maximum(top, t)
    top = jnp.max(top, axis=0, keepdims=True)
    total = None
    for i in range(keys // step):
        e = jnp.exp2((s_scr[i * step : (i + 1) * step, :] - top) * LOG2E)
        t = jnp.sum(e.reshape(step // 8, 8, queries), axis=0)
        total = t if total is None else total + t
        e_ref[0, i * step : (i + 1) * step, :] = e.astype(BF16)
    l_ref[0] = jnp.sum(total, axis=0, keepdims=True)


def attend(sv_ref, sb_ref, meta_ref, *refs):
    (
        own, other, kq_ref, e_ref, l_ref, g_ref, kv_ref, o_ref, near_ref, far_ref,
        kq_scr, v_scr, turned_scr, g_scr, acc, sem,
    ) = refs
    views = kq_scr.shape[1]
    view = pl.program_id(0)

    @pl.when(view == 0)
    def _():
        c = meta_ref[0]
        copies = [
            pltpu.make_async_copy(kq_ref, kq_scr, sem.at[0]),
            pltpu.make_async_copy(own.at[:, pl.ds(0, v_scr.shape[2])], v_scr.at[c], sem.at[1]),
            pltpu.make_async_copy(
                other.at[:, pl.ds(0, v_scr.shape[2])], v_scr.at[1 - c], sem.at[2]
            ),
        ]
        for copy in copies:
            copy.start()
        for copy in copies:
            copy.wait()
        acc[...] = jnp.zeros_like(acc)
        rows = v_scr.shape[2]
        for half in range(2):
            for source in range(views):
                v = v_scr[half, source]
                k = kq_scr[half, source]
                kv_ref[half, source, :rows, :] = join(k[:rows], v)
                kv_ref[half, source, rows:, :] = jnp.concatenate(
                    [k[rows:, :HEAD_DIM], v[:, HEAD_DIM:]], axis=1
                )

    gather(sv_ref, sb_ref, view, kv_ref, None, turned_scr)
    out = dot(turned_scr[...], e_ref[0])[HEAD_DIM:] / l_ref[0]
    o_ref[0] = fold(out).astype(BF16)
    g = (unfold(g_ref[0]).astype(F32) / l_ref[0]).astype(BF16)
    zero = jnp.zeros_like(g)
    g_scr[0] = jnp.concatenate([g, zero], axis=0).T
    g_scr[1] = jnp.concatenate([zero, g], axis=0).T
    scatter_folded(sv_ref, sb_ref, view, acc, e_ref.at[0], g_scr)

    @pl.when(view == pl.num_programs(0) - 1)
    def _():
        hand_back_views(meta_ref, acc, near_ref, far_ref)


def backward(
    sv_ref, sb_ref, meta_ref, kv_ref, kq_ref, e_ref, o_ref, l_ref, g_ref,
    dq_ref, near_ref, far_ref, kv_scr, q_scr, rows_scr, turned_scr, ds_scr, qz_scr, acc, sem,
):
    view = pl.program_id(0)

    @pl.when(view == 0)
    def _():
        first = pltpu.make_async_copy(kv_ref, kv_scr, sem.at[0])
        second = pltpu.make_async_copy(kq_ref.at[meta_ref[0]], q_scr, sem.at[1])
        first.start()
        second.start()
        acc[...] = jnp.zeros_like(acc)
        first.wait()
        second.wait()

    gather(sv_ref, sb_ref, view, kv_scr, rows_scr, turned_scr)
    keys, _ = ds_scr.shape
    step = 256
    q = q_scr[view].T[HEAD_DIM:] * jnp.asarray(SCALE, BF16)
    zero = jnp.zeros_like(q)
    qz_scr[0] = jnp.concatenate([q, zero], axis=0).T
    qz_scr[1] = jnp.concatenate([zero, q], axis=0).T
    g = (unfold(g_ref[0]).astype(F32) / l_ref[0]).astype(BF16)
    delta = jnp.sum(unfold(o_ref[0]).astype(F32) * g.astype(F32), axis=0, keepdims=True)
    g = jnp.concatenate([zero, g], axis=0)
    for i in range(keys // step):
        rows = slice(i * step, (i + 1) * step)
        dp = dot(rows_scr[rows, :], g)
        ds_scr[rows, :] = (e_ref[0, rows, :].astype(F32) * (dp - delta)).astype(BF16)
    scatter_folded(sv_ref, sb_ref, view, acc, ds_scr, qz_scr)
    dq = dot(turned_scr[...], ds_scr[...])[:HEAD_DIM] * SCALE
    dq_ref[0] = jnp.concatenate([jnp.zeros_like(dq), dq], axis=0).T.astype(BF16)

    @pl.when(view == pl.num_programs(0) - 1)
    def _():
        hand_back(meta_ref, acc, near_ref, far_ref)


def combine_kq(meta_ref, near_ref, far_ref, dq_ref, *outs):
    count = len(outs) // 2
    rows = near_ref.shape[1]
    for n, (out, (j, i)) in enumerate(zip(outs, messages(count))):
        dk = (near_ref[n] + far_ref[n].astype(F32)).astype(BF16)
        dq = dq_ref[source_of(meta_ref, meta_ref[0], j, i, count)]
        out[:rows, :] = jnp.concatenate([dk[:, :HEAD_DIM], dq[:rows, HEAD_DIM:]], axis=1)
        out[rows:, :] = join_high(dk, dq[rows:])


def plane_body(query_rows, key_rows, value_rows, out_weight, out_grad, source_view, source_block):
    tokens, columns = query_rows.shape
    half = tokens // 2
    count = columns // HEAD_DIM
    views = 2 * count
    keys = source_view.shape[1] * BLOCK_TOKENS
    group = lax.axis_size("head")
    head_index = lax.axis_index("head").astype(jnp.int32)
    view_index = lax.axis_index("view").astype(jnp.int32)
    core = lax.rem(head_index, 2)
    meta = jnp.stack([core, lax.rem(view_index, count), lax.div(view_index, count)])
    spot = jnp.stack([lax.div(head_index, 2), head_index])
    routes = (source_view, source_block, meta)

    def flip(x, bits):
        return lax.ppermute(x, "head", [(n, n ^ bits) for n in range(group)])

    def view_swap(x):
        return lax.all_to_all(x, "view", split_axis=0, concat_axis=0, tiled=True)

    def pairs_of(j, i):
        for v in range(views):
            for h in range(group):
                to = (h % 2) * count + ((v % count) ^ j)
                yield v * group + h, to * group + (h - h % 2) + ((v // count) ^ i)

    def send(parts, back=False):
        out = []
        for part, (j, i) in zip(parts, messages(count)):
            pairs = [(b, a) if back else (a, b) for a, b in pairs_of(j, i)]
            out.append(lax.ppermute(part, ("view", "head"), pairs))
        return out

    full = whole(tokens, columns)
    wide, wide_shape = whole(half, 128), shape_of(half, 128)
    thin, thin_shape = whole(count, half // 2, 128), shape_of(count, half // 2, 128)
    kq = call(
        pack_kq, (meta,), (query_rows, key_rows), [full] * 2, [wide] * views, [wide_shape] * views
    )
    kq = send(kq)
    v, v_give = call(pack_v, (meta,), (value_rows,), [full], [thin] * 2, [thin_shape] * 2)
    v_got = flip(v_give, 1)
    first = core == 0
    og_keep = lax.dynamic_slice_in_dim(out_grad, core * half, half, 0)
    og_give = lax.dynamic_slice_in_dim(out_grad, (1 - core) * half, half, 0)
    og = [og_keep, flip(og_give, 1), flip(og_keep, 2), flip(og_give, 3)]
    g = call(
        attended_grads,
        (spot,),
        (*og, v, v_got, out_weight),
        [whole(half, columns)] * group
        + [thin] * 2
        + [pl.BlockSpec((views * HEAD_DIM, group * columns), lambda i, s: (s[0], 0))],
        whole(views, half, 128),
        shape_of(views, half, 128),
    )
    vg = view_swap(g)
    kq_other = [flip(x, 1) for x in kq]
    vg_other = flip(vg, 1)
    per_view_e = pl.BlockSpec((1, keys, half), lambda i, *_: (i, 0, 0))
    per_view_l = pl.BlockSpec((1, 1, half), lambda i, *_: (i, 0, 0))
    per_view = pl.BlockSpec((1, half // 2, 128), lambda i, *_: (i, 0, 0))
    per_view_g = pl.BlockSpec((1, half // 2, 128), lambda i, *_: (i, 1, 0))
    all_rows = whole(2, views, half, 128)
    unit = 2 * views * keys * half * 64
    kq_all, e, l = call(
        scores,
        routes,
        (*kq, *kq_other),
        [HBM] * (2 * views),
        [all_rows, per_view_e, per_view_l],
        [
            shape_of(2, views, half, 128),
            shape_of(views, keys, half),
            shape_of(views, 1, half, dtype=F32),
        ],
        grid=(views,),
        scratch=[
            pltpu.VMEM((keys, 128), BF16),
            pltpu.VMEM((keys, half), F32),
            pltpu.SemaphoreType.DMA((2 * views,)),
        ],
        flops=unit * 4,
    )
    folded = whole(views, half // 2, 128)
    near_far = [shape_of(views, half // 2, 128, dtype=F32), shape_of(views, half // 2, 128)]
    kv_all, o, near_v, far_v = call(
        attend,
        routes,
        (vg, vg_other, kq_all, e, l, vg),
        [HBM] * 3 + [per_view_e, per_view_l, per_view_g],
        [all_rows, per_view, folded, folded],
        [shape_of(2, views, half, 128), shape_of(views, half // 2, 128), *near_far],
        grid=(views,),
        scratch=[
            pltpu.VMEM((2, views, half, 128), BF16),
            pltpu.VMEM((2, views, half // 2, 128), BF16),
            pltpu.VMEM((128, keys), BF16),
            pltpu.VMEM((2, half, 128), BF16),
            pltpu.VMEM((2, views, half // 2, 128), F32),
            pltpu.SemaphoreType.DMA((3,)),
        ],
        flops=unit * 3,
    )
    far_v = flip(far_v, 1)
    dvo = call(
        combine_v, (), (near_v, far_v, o), [folded] * 3, whole(views, half, 128),
        shape_of(views, half, 128),
    )
    dvo = view_swap(dvo)
    dq, near_k, far_k = call(
        backward,
        routes,
        (kv_all, kq_all, e, o, l, vg),
        [HBM, HBM, per_view_e, per_view, per_view_l, per_view_g],
        [pl.BlockSpec((1, half, 128), lambda i, *_: (i, 0, 0)), folded, folded],
        [shape_of(views, half, 128), *near_far],
        grid=(views,),
        scratch=[
            pltpu.VMEM((2, views, half, 128), BF16),
            pltpu.VMEM((views, half, 128), BF16),
            pltpu.VMEM((keys, 128), BF16),
            pltpu.VMEM((128, keys), BF16),
            pltpu.VMEM((keys, half), BF16),
            pltpu.VMEM((2, half, 128), BF16),
            pltpu.VMEM((2, views, half // 2, 128), F32),
            pltpu.SemaphoreType.DMA((2,)),
        ],
        flops=unit * 8,
    )
    far_k = flip(far_k, 1)
    dkq = call(
        combine_kq,
        (meta,),
        (near_k, far_k, dq),
        [folded, folded, whole(views, half, 128)],
        [wide] * views,
        [wide_shape] * views,
    )
    dkq = send(dkq, back=True)
    o_other = flip(lax.slice_in_dim(dvo, half // 2, half, axis=1), 2)
    mixed, mixed_give = call(
        mix,
        (spot,),
        (dvo, o_other, out_weight),
        [
            pl.BlockSpec((views, half // 2, 128), lambda i, s: (0, 1, 0)),
            folded,
            pl.BlockSpec((group * columns, 2 * columns), lambda i, s: (0, s[0])),
        ],
        [whole(half, columns)] * 2,
        [shape_of(half, columns)] * 2,
    )
    mixed_got = flip(mixed_give, 1)
    mixed_out = jnp.concatenate(
        [jnp.where(first, mixed, mixed_got), jnp.where(first, mixed_got, mixed)], axis=0
    )
    give = lax.slice_in_dim(dvo, 0, half // 2, axis=1)
    dv_got = flip(lax.dynamic_slice_in_dim(give, (1 - core) * count, count, 0), 1)
    value_grad = call(
        unpack_v, (meta,), (dvo, dv_got), [HBM] * 2, full, shape_of(tokens, columns),
        scratch=[
            pltpu.VMEM((2, count, half // 2, 128), BF16), pltpu.SemaphoreType.DMA((2,))
        ],
    )
    query_grad, key_grad = call(
        unpack_kq, (meta,), tuple(dkq), [HBM] * views, [full] * 2,
        [shape_of(tokens, columns)] * 2,
        scratch=[
            pltpu.VMEM((2, count, half, 128), BF16), pltpu.SemaphoreType.DMA((views,))
        ],
    )
    return mixed_out, query_grad, key_grad, value_grad


def score_rows(query_part, key_heads, score_scale):
    return (
        jnp.einsum("qhd,khd->hqk", query_part, key_heads, preferred_element_type=jnp.float32)
        * score_scale
    )


def body(query_rows, key_rows, value_rows, out_weight, out_grad, source_view, source_block):
    tokens = query_rows.shape[0]
    columns = query_rows.shape[1]
    heads_here = columns // HEAD_DIM
    slot_count = source_view.shape[1]
    key_count = slot_count * BLOCK_TOKENS
    peer_count = lax.axis_size("view")
    capacity = max(1, 2 * slot_count // peer_count)
    block_count = tokens // BLOCK_TOKENS
    view_index = lax.axis_index("view")
    head_index = lax.axis_index("head")
    score_scale = HEAD_DIM ** (-0.5)
    slot_order = jnp.arange(slot_count, dtype=jnp.int32)
    same_view = source_view[:, :, None] == source_view[:, None, :]
    earlier = slot_order[None, :] < slot_order[:, None]
    slot_rank = jnp.sum((same_view & earlier[None]).astype(jnp.int32), axis=2)
    copy_order = jnp.arange(capacity, dtype=jnp.int32)
    matched = (source_view == view_index)[:, :, None] & (
        slot_rank[:, :, None] == copy_order[None, None, :]
    )
    filled = jnp.any(matched, axis=1)
    chosen = jnp.sum(jnp.where(matched, source_block[:, :, None], 0), axis=1)
    own_view = lax.dynamic_index_in_dim(source_view, view_index, 0, keepdims=False)
    own_rank = lax.dynamic_index_in_dim(slot_rank, view_index, 0, keepdims=False)
    landing = own_view * capacity + own_rank
    joined = jnp.concatenate([key_rows, value_rows], axis=1)
    outgoing = jnp.take(
        joined.reshape(block_count, BLOCK_TOKENS, 2 * columns), chosen.reshape(-1), axis=0
    )
    outgoing = outgoing.reshape(peer_count, capacity, BLOCK_TOKENS, 2 * columns)
    incoming = lax.all_to_all(outgoing, "view", split_axis=0, concat_axis=0, tiled=True)
    fetched = jnp.take(
        incoming.reshape(peer_count * capacity, BLOCK_TOKENS, 2 * columns), landing, axis=0
    )
    fetched = fetched.reshape(key_count, 2 * columns)
    query_block = min(512, tokens)
    block_total = tokens // query_block
    key_heads = fetched[:, :columns].reshape(key_count, heads_here, HEAD_DIM)
    value_heads = fetched[:, columns:].reshape(key_count, heads_here, HEAD_DIM)
    query_heads = query_rows.reshape(block_total, query_block, heads_here, HEAD_DIM)

    def forward_step(query_part):
        scores = score_rows(query_part, key_heads, score_scale)
        row_top = jnp.max(scores, axis=-1, keepdims=True)
        shifted = jnp.exp(scores - row_top)
        row_total = jnp.sum(shifted, axis=-1, keepdims=True)
        weights = (shifted / row_total).astype(jnp.bfloat16)
        out_part = jnp.einsum(
            "hqk,khd->qhd", weights, value_heads, preferred_element_type=jnp.float32
        )
        return (out_part.astype(jnp.bfloat16), row_top, row_total)

    attended, row_tops, row_totals = lax.map(forward_step, query_heads)
    attended_rows = attended.reshape(tokens, columns)
    own_rows = lax.dynamic_slice_in_dim(out_weight, head_index * columns, columns, 0)
    part_weight = own_rows
    summed_rows = lax.psum_scatter(
        lax.dot_general(
            part_weight, attended_rows, (((0,), (1,)), ((), ())), preferred_element_type=jnp.float32
        ).astype(jnp.bfloat16),
        "head",
        scatter_dimension=0,
        tiled=True,
    ).astype(jnp.float32)
    mixed_out = summed_rows.T.astype(jnp.bfloat16)
    part_weight = own_rows
    attended_grad = lax.dot_general(
        lax.all_gather(out_grad, "head", axis=1, tiled=True),
        part_weight,
        (((1,), (1,)), ((), ())),
        preferred_element_type=jnp.float32,
    )
    grad_heads = attended_grad.astype(jnp.bfloat16).reshape(
        block_total, query_block, heads_here, HEAD_DIM
    )

    def backward_step(totals, inputs):
        key_total, value_total = totals
        query_part, out_part, grad_part, row_top, row_total = inputs
        scores = score_rows(query_part, key_heads, score_scale)
        probability = jnp.exp(scores - row_top) / row_total
        weights = probability.astype(jnp.bfloat16)
        grad_prob = jnp.einsum(
            "qhd,khd->hqk", grad_part, value_heads, preferred_element_type=jnp.float32
        )
        row_delta = jnp.einsum(
            "qhd,qhd->hq", out_part, grad_part, preferred_element_type=jnp.float32
        )[:, :, None]
        grad_scores = (probability * (grad_prob - row_delta)).astype(jnp.bfloat16)
        query_part_grad = (
            jnp.einsum("hqk,khd->qhd", grad_scores, key_heads, preferred_element_type=jnp.float32)
            * score_scale
        )
        key_total = (
            key_total
            + jnp.einsum(
                "hqk,qhd->khd", grad_scores, query_part, preferred_element_type=jnp.float32
            )
            * score_scale
        )
        value_total = value_total + jnp.einsum(
            "hqk,qhd->khd", weights, grad_part, preferred_element_type=jnp.float32
        )
        return ((key_total, value_total), query_part_grad.astype(jnp.bfloat16))

    zero_keys = jnp.zeros((key_count, heads_here, HEAD_DIM), jnp.float32)
    (key_total, value_total), query_grads = lax.scan(
        backward_step,
        (zero_keys, zero_keys),
        (query_heads, attended, grad_heads, row_tops, row_totals),
    )
    query_grad = query_grads.reshape(tokens, columns)
    slot_grads = jnp.concatenate(
        [key_total.reshape(key_count, columns), value_total.reshape(key_count, columns)], axis=1
    )
    slot_grads = slot_grads.reshape(slot_count, BLOCK_TOKENS * 2 * columns)
    placing = (
        landing[None, :] == jnp.arange(peer_count * capacity, dtype=jnp.int32)[:, None]
    ).astype(jnp.float32)
    outgoing_grads = jnp.dot(placing, slot_grads, precision=lax.Precision.HIGHEST).reshape(
        peer_count, capacity, BLOCK_TOKENS, 2 * columns
    )
    returned = lax.all_to_all(
        outgoing_grads.astype(jnp.bfloat16), "view", split_axis=0, concat_axis=0, tiled=True
    ).astype(outgoing_grads.dtype)
    gathering = (
        chosen.reshape(-1)[None, :] == jnp.arange(block_count, dtype=jnp.int32)[:, None]
    ) & filled.reshape(-1)[None, :]
    summed = jnp.dot(
        gathering.astype(jnp.float32),
        returned.reshape(peer_count * capacity, BLOCK_TOKENS * 2 * columns),
        precision=lax.Precision.HIGHEST,
    )
    summed = summed.reshape(tokens, 2 * columns)
    key_grad = summed[:, :columns].astype(jnp.bfloat16)
    value_grad = summed[:, columns:].astype(jnp.bfloat16)
    return (mixed_out, query_grad, key_grad, value_grad)


def planes(*args):
    return plane_body(*args)


def solution(mesh):
    placed = P("view", "head")
    views, group = mesh.shape["view"], mesh.shape["head"]

    def step(*args):
        tokens, columns = args[0].shape
        count = columns // group // HEAD_DIM
        fits = (
            group == 4
            and views == 2 * count
            and count & (count - 1) == 0
            and tokens // views % (4 * BLOCK_TOKENS) == 0
        )
        inner = jax.shard_map(
            planes if fits else body,
            mesh=mesh,
            in_specs=(placed, placed, placed, P(), placed, P(), P()),
            out_specs=(placed,) * 4,
            check_vma=False,
        )
        return inner(*args)

    return step
```

```python
import jax
import jax.numpy as jnp
from jax import lax
from jax.experimental import pallas as pl
from jax.experimental.pallas import tpu as pltpu
from jax.sharding import PartitionSpec as P


HEAD_DIM = 64
BLOCK_TOKENS = 128
SCALE = HEAD_DIM**-0.5
LOG2E = 1.4426950408889634
F32 = jnp.float32
BF16 = jnp.bfloat16
HBM = pl.BlockSpec(memory_space=pl.ANY)
STEP = 256


def join(a, b):
    return jnp.concatenate([a[:, :HEAD_DIM], b[:, :HEAD_DIM]], axis=1)


def join_high(a, b):
    return jnp.concatenate([a[:, HEAD_DIM:], b[:, HEAD_DIM:]], axis=1)


def dot(a, b):
    return jnp.dot(a, b, preferred_element_type=F32)


def aligned(index, size):
    return pl.ds(pl.multiple_of(index * size, size), size)


def call(kernel, scalars, args, in_specs, out_specs, out_shape, grid=(1,), scratch=(), flops=0):
    return pl.pallas_call(
        kernel,
        grid_spec=pltpu.PrefetchScalarGridSpec(
            num_scalar_prefetch=len(scalars),
            grid=grid,
            in_specs=in_specs,
            out_specs=out_specs,
            scratch_shapes=list(scratch),
        ),
        out_shape=out_shape,
        compiler_params=pltpu.CompilerParams(dimension_semantics=("arbitrary",) * len(grid)),
        cost_estimate=pl.CostEstimate(flops=flops, transcendentals=0, bytes_accessed=0)
        if flops
        else None,
    )(*scalars, *args)


def whole(*shape):
    return pl.BlockSpec(shape, lambda *_: (0,) * len(shape))


def shape_of(*shape, dtype=BF16):
    return jax.ShapeDtypeStruct(shape, dtype)


def run_copies(*copies):
    for copy in copies:
        copy.start()
    for copy in copies:
        copy.wait()


def fold_all(x_ref, out_ref):
    rows, columns = x_ref.shape
    count = columns // HEAD_DIM
    for head in range(0, count, 2):
        lanes = slice(HEAD_DIM * head, HEAD_DIM * (head + 2))
        top, low = x_ref[: rows // 2, lanes], x_ref[rows // 2 :, lanes]
        for n in range(head, out_ref.shape[0], count):
            out_ref[n] = join(top, low)
            out_ref[n + 1] = join_high(top, low)


def fold_each(meta_ref, x_ref, outs):
    rows = x_ref.shape[0]
    for n, out in enumerate(outs):
        head = meta_ref[0] ^ n
        pair = aligned(head // 2, 128)
        top, low = x_ref[: rows // 2, pair], x_ref[rows // 2 :, pair]
        out[...] = jnp.where(head % 2 == 1, join_high(top, low), join(top, low))


def pack_k(x_ref, out_ref):
    fold_all(x_ref, out_ref)


def pack_v(x_ref, out_ref):
    fold_all(x_ref, out_ref)


def pack_q(meta_ref, x_ref, *outs):
    fold_each(meta_ref, x_ref, outs)


def spread(parts, out_ref):
    rows = out_ref.shape[0] // 2
    for head in range(0, len(parts), 2):
        lanes = slice(HEAD_DIM * head, HEAD_DIM * (head + 2))
        out_ref[:rows, lanes] = join(parts[head], parts[head + 1])
        out_ref[rows:, lanes] = join_high(parts[head], parts[head + 1])


def collect(meta_ref, *refs):
    parts, (out_ref, scr, sem) = refs[:-3], refs[-3:]
    run_copies(
        *(
            pltpu.make_async_copy(part, scr.at[meta_ref[0] ^ n], sem.at[n])
            for n, part in enumerate(parts)
        )
    )
    spread([scr[n] for n in range(len(parts))], out_ref)


def total_of(x_ref, out_ref):
    count = out_ref.shape[1] // HEAD_DIM
    parts = []
    for head in range(count):
        part = x_ref[head].astype(F32)
        for n in range(head + count, x_ref.shape[0], count):
            part = part + x_ref[n].astype(F32)
        parts.append(part.astype(BF16))
    spread(parts, out_ref)


def total_k(meta_ref, *refs):
    parts, (out_ref, scr, sem) = refs[:-3], refs[-3:]
    count = out_ref.shape[1] // HEAD_DIM
    run_copies(
        *(
            pltpu.make_async_copy(
                part, scr.at[n // count * count + (meta_ref[0] ^ (n % count))], sem.at[n]
            )
            for n, part in enumerate(parts)
        )
    )
    total_of(scr, out_ref)


def total_v(x_ref, out_ref):
    total_of(x_ref, out_ref)


def attended_grads(meta_ref, own_ref, *refs):
    count = own_ref.shape[1] // HEAD_DIM
    outs, scr = refs[-1 - count : -1], refs[-1]
    parts, w_ref = (own_ref, *refs[: -2 - count]), refs[-2 - count]
    columns = own_ref.shape[1]
    total = None
    for n, part in enumerate(parts):
        piece = lax.dot_general(
            part[...],
            w_ref[:, aligned(meta_ref[2] ^ n, columns)],
            (((1,), (1,)), ((), ())),
            preferred_element_type=F32,
        )
        total = piece if total is None else total + piece
    scr[...] = total.astype(BF16)
    fold_each(meta_ref, scr, outs)


def mix(meta_ref, *refs):
    parts, (w_ref, out_ref) = refs[:-2], refs[-2:]
    columns = out_ref.shape[1]
    total = None
    for n, part in enumerate(parts):
        piece = dot(part[...], w_ref[aligned(meta_ref[2] ^ n, columns), :])
        total = piece if total is None else total + piece
    out_ref[...] = total.astype(BF16)


def place(sv_ref, sb_ref, view, slot, per_half):
    block = sb_ref[view, slot]
    return sv_ref[view, slot], lax.div(block, per_half), aligned(lax.rem(block, per_half), BLOCK_TOKENS)


def gather(sv_ref, sb_ref, view, src, rows_scr=None, turned_scr=None):
    per_half = src.shape[1] // BLOCK_TOKENS
    for slot in range(sv_ref.shape[1]):
        source, high, rows = place(sv_ref, sb_ref, view, slot, per_half)
        block = src[source, rows, :]
        block = jnp.where(high == 1, join_high(block, block), block)
        span = slice(slot * BLOCK_TOKENS, (slot + 1) * BLOCK_TOKENS)
        if rows_scr is not None:
            rows_scr[span, :] = block
        if turned_scr is not None:
            turned_scr[:, span] = block.T[:HEAD_DIM]


def scatter(sv_ref, sb_ref, view, acc, lhs, rhs):
    per_view = acc.shape[1] // BLOCK_TOKENS
    keys = sv_ref.shape[1] * BLOCK_TOKENS
    for start in range(0, keys, STEP):
        part = None
        for a, b in zip(lhs, rhs):
            piece = dot(a[start : start + STEP, :], b)
            part = piece if part is None else part + piece
        for inner in range(0, STEP, BLOCK_TOKENS):
            source, _, rows = place(sv_ref, sb_ref, view, (start + inner) // BLOCK_TOKENS, per_view)
            acc[source, rows, :] += part[inner : inner + BLOCK_TOKENS]


def give_back(acc, out_ref):
    rows = out_ref.shape[1]
    for view in range(acc.shape[0]):
        block = acc[view].astype(BF16)
        out_ref[view] = join(block[:rows], block[rows:])


def halves(block):
    t = block.T
    return [t[:HEAD_DIM], t[HEAD_DIM:]]


def padded(t):
    return jnp.concatenate([t, jnp.zeros_like(t)], axis=0)


def scores(sv_ref, sb_ref, meta_ref, k_ref, *refs):
    count = len(refs) - 8
    parts = refs[:count]
    e_ref, l_ref, k_scr, q_scr, rows_scr, s0, s1, sem = refs[count:]
    step = pl.program_id(0)

    @pl.when(step == 0)
    def _():
        run_copies(
            pltpu.make_async_copy(k_ref, k_scr, sem.at[count]),
            *(pltpu.make_async_copy(p, q_scr.at[n], sem.at[n]) for n, p in enumerate(parts)),
        )

    view = meta_ref[1] * count + (meta_ref[0] ^ step)
    gather(sv_ref, sb_ref, view, k_scr, rows_scr=rows_scr)
    keys, queries = s0.shape
    tops = []
    for t, s_scr in zip(halves(q_scr[step]), (s0, s1)):
        q = padded(t * jnp.asarray(SCALE, BF16))
        top = None
        for i in range(0, keys, STEP):
            s = dot(rows_scr[i : i + STEP, :], q)
            s_scr[i : i + STEP, :] = s
            m = jnp.max(s.reshape(STEP // 8, 8, queries), axis=0)
            top = m if top is None else jnp.maximum(top, m)
        tops.append(jnp.max(top, axis=0, keepdims=True))
    for n, (top, s_scr) in enumerate(zip(tops, (s0, s1))):
        total = None
        for i in range(0, keys, STEP):
            e = jnp.exp2((s_scr[i : i + STEP, :] - top) * LOG2E)
            m = jnp.sum(e.reshape(STEP // 8, 8, queries), axis=0)
            total = m if total is None else total + m
            e_ref[0, n, i : i + STEP, :] = e.astype(BF16)
        l_ref[0, n] = jnp.sum(total, axis=0, keepdims=True)


def attend(sv_ref, sb_ref, meta_ref, v_ref, *refs):
    count = (len(refs) - 9) // 2
    parts, outs = refs[:count], refs[count + 2 : 2 * count + 2]
    e_ref, l_ref = refs[count : count + 2]
    delta_ref, dv_ref, v_scr, g_scr, turned_scr, acc, sem = refs[2 * count + 2 :]
    step = pl.program_id(0)

    @pl.when(step == 0)
    def _():
        run_copies(
            pltpu.make_async_copy(v_ref, v_scr, sem.at[count]),
            *(pltpu.make_async_copy(p, g_scr.at[n], sem.at[n]) for n, p in enumerate(parts)),
        )
        acc[...] = jnp.zeros_like(acc)

    view = meta_ref[1] * count + (meta_ref[0] ^ step)
    gather(sv_ref, sb_ref, view, v_scr, turned_scr=turned_scr)
    out, grads = [], []
    for n, g in enumerate(halves(g_scr[step])):
        o = (dot(turned_scr[...], e_ref[0, n]) / l_ref[0, n]).astype(BF16)
        g = (g.astype(F32) / l_ref[0, n]).astype(BF16)
        delta_ref[0, n] = jnp.sum(o.astype(F32) * g.astype(F32), axis=0, keepdims=True)
        out.append(o)
        grads.append(padded(g).T)
    out = jnp.concatenate(out, axis=0).T
    for n, ref in enumerate(outs):

        @pl.when(step == n)
        def _():
            ref[...] = out

    scatter(sv_ref, sb_ref, view, acc, (e_ref.at[0, 0], e_ref.at[0, 1]), grads)

    @pl.when(step == count - 1)
    def _():
        give_back(acc, dv_ref)


def backward(sv_ref, sb_ref, meta_ref, k_ref, v_ref, *refs):
    k_scr, v_scr, q_scr, g_scr, rows_scr, turned_scr, ds0, ds1, acc, sem = refs[-10:]
    count = q_scr.shape[0]
    q_parts, g_parts = refs[:count], refs[count : 2 * count]
    e_ref, l_ref, delta_ref = refs[2 * count : 2 * count + 3]
    outs = refs[2 * count + 3 : 3 * count + 3]
    dk_refs = refs[3 * count + 3 : -10]
    step = pl.program_id(0)

    @pl.when(step == 0)
    def _():
        run_copies(
            pltpu.make_async_copy(k_ref, k_scr, sem.at[2 * count]),
            pltpu.make_async_copy(v_ref, v_scr, sem.at[2 * count + 1]),
            *(pltpu.make_async_copy(p, q_scr.at[n], sem.at[n]) for n, p in enumerate(q_parts)),
            *(
                pltpu.make_async_copy(p, g_scr.at[n], sem.at[count + n])
                for n, p in enumerate(g_parts)
            ),
        )
        acc[...] = jnp.zeros_like(acc)

    view = meta_ref[1] * count + (meta_ref[0] ^ step)
    gather(sv_ref, sb_ref, view, v_scr, rows_scr=rows_scr)
    gather(sv_ref, sb_ref, view, k_scr, turned_scr=turned_scr)
    keys = rows_scr.shape[0]
    queries = [padded(t * jnp.asarray(SCALE, BF16)).T for t in halves(q_scr[step])]
    for n, (g, ds_scr) in enumerate(zip(halves(g_scr[step]), (ds0, ds1))):
        g = padded((g.astype(F32) / l_ref[0, n]).astype(BF16))
        for i in range(0, keys, STEP):
            dp = dot(rows_scr[i : i + STEP, :], g)
            e = e_ref[0, n, i : i + STEP, :].astype(F32)
            ds_scr[i : i + STEP, :] = (e * (dp - delta_ref[0, n])).astype(BF16)
    scatter(sv_ref, sb_ref, view, acc, (ds0, ds1), queries)
    dq = [(dot(turned_scr[...], ds[...]) * SCALE).astype(BF16) for ds in (ds0, ds1)]
    dq = jnp.concatenate(dq, axis=0).T
    for n, ref in enumerate(outs):

        @pl.when(step == n)
        def _():
            ref[...] = dq

    @pl.when(step == count - 1)
    def _():
        for n, ref in enumerate(dk_refs):
            rows = ref.shape[0]
            block = acc[(meta_ref[1] * count + meta_ref[0]) ^ n].astype(BF16)
            ref[...] = join(block[:rows], block[rows:])


def plane_body(query_rows, key_rows, value_rows, out_weight, out_grad, source_view, source_block):
    tokens, columns = query_rows.shape
    half = tokens // 2
    count = columns // HEAD_DIM
    views = lax.axis_size("view")
    group = lax.axis_size("head")
    keys = source_view.shape[1] * BLOCK_TOKENS
    head_index = lax.axis_index("head").astype(jnp.int32)
    view_index = lax.axis_index("view").astype(jnp.int32)
    meta = jnp.stack([lax.rem(view_index, count), lax.div(view_index, count), head_index])
    routes = (source_view, source_block, meta)

    def gathered(x):
        return [x] + [
            lax.ppermute(x, "head", [(n, n ^ bits) for n in range(group)])
            for bits in range(1, group)
        ]

    def view_swap(x):
        return lax.all_to_all(x, "view", split_axis=0, concat_axis=0, tiled=True)

    def send(parts):
        return [parts[0]] + [
            lax.ppermute(part, "view", [(n, n ^ bits) for n in range(views)])
            for bits, part in enumerate(parts)
            if bits
        ]

    full, rows_shape = whole(tokens, columns), shape_of(tokens, columns)
    one, one_shape = whole(half, 128), shape_of(half, 128)
    every, every_shape = whole(views, half, 128), shape_of(views, half, 128)
    k = call(pack_k, (), (key_rows,), [full], every, every_shape)
    k = view_swap(k)
    q = call(pack_q, (meta,), (query_rows,), [full], [one] * count, [one_shape] * count)
    q = send(q)
    og = gathered(out_grad)
    v = call(pack_v, (), (value_rows,), [full], every, every_shape)
    v = view_swap(v)
    g = call(
        attended_grads,
        (meta,),
        (*og, out_weight),
        [full] * group + [pl.BlockSpec((columns, group * columns), lambda i, m: (m[2], 0))],
        [one] * count,
        [one_shape] * count,
        scratch=[pltpu.VMEM((tokens, columns), BF16)],
    )
    g = send(g)
    e_spec = pl.BlockSpec((1, 2, keys, half), lambda i, *_: (i, 0, 0, 0))
    row_spec = pl.BlockSpec((1, 2, 1, half), lambda i, *_: (i, 0, 0, 0))
    row_shape = shape_of(count, 2, 1, half, dtype=F32)
    unit = 2 * count * keys * tokens * HEAD_DIM
    held = pltpu.VMEM((views, half, 128), BF16)
    mine = pltpu.VMEM((count, half, 128), BF16)
    totals = pltpu.VMEM((views, tokens, 128), F32)
    rows_scr = pltpu.VMEM((keys, 128), BF16)
    turned_scr = pltpu.VMEM((HEAD_DIM, keys), BF16)
    e, l = call(
        scores,
        routes,
        (k, *q),
        [HBM] * (1 + count),
        [e_spec, row_spec],
        [shape_of(count, 2, keys, half), row_shape],
        grid=(count,),
        scratch=[
            held, mine, rows_scr, pltpu.VMEM((keys, half), F32), pltpu.VMEM((keys, half), F32),
            pltpu.SemaphoreType.DMA((count + 1,)),
        ],
        flops=unit * 4,
    )
    *o, delta, dv = call(
        attend,
        routes,
        (v, *g, e, l),
        [HBM] * (1 + count) + [e_spec, row_spec],
        [one] * count + [row_spec, every],
        [one_shape] * count + [row_shape, every_shape],
        grid=(count,),
        scratch=[held, mine, turned_scr, totals, pltpu.SemaphoreType.DMA((count + 1,))],
        flops=unit * 3,
    )
    dv = view_swap(dv)
    o = send(o)
    back = call(
        backward,
        routes,
        (k, v, *q, *g, e, l, delta),
        [HBM] * (2 + 2 * count) + [e_spec, row_spec, row_spec],
        [one] * (count + views),
        [one_shape] * (count + views),
        grid=(count,),
        scratch=[
            held, held, mine, mine, rows_scr, turned_scr,
            pltpu.VMEM((keys, half), BF16), pltpu.VMEM((keys, half), BF16),
            totals, pltpu.SemaphoreType.DMA((2 * count + 2,)),
        ],
        flops=unit * 8,
    )
    dk = send(back[count:])
    dq = send(back[:count])

    def collected(parts):
        return call(
            collect, (meta,), tuple(parts), [HBM] * count, full, rows_shape,
            scratch=[mine, pltpu.SemaphoreType.DMA((count,))],
        )

    attended = collected(o)
    attended = gathered(attended)
    mixed_out = call(
        mix,
        (meta,),
        (*attended, out_weight),
        [full] * group + [pl.BlockSpec((group * columns, columns), lambda i, m: (0, m[2]))],
        full,
        rows_shape,
    )
    value_grad = call(total_v, (), (dv,), [every], full, rows_shape)
    query_grad = collected(dq)
    key_grad = call(
        total_k, (meta,), tuple(dk), [HBM] * views, full, rows_shape,
        scratch=[held, pltpu.SemaphoreType.DMA((views,))],
    )
    return mixed_out, query_grad, key_grad, value_grad


def score_rows(query_part, key_heads, score_scale):
    return (
        jnp.einsum("qhd,khd->hqk", query_part, key_heads, preferred_element_type=jnp.float32)
        * score_scale
    )


def body(query_rows, key_rows, value_rows, out_weight, out_grad, source_view, source_block):
    tokens = query_rows.shape[0]
    columns = query_rows.shape[1]
    heads_here = columns // HEAD_DIM
    slot_count = source_view.shape[1]
    key_count = slot_count * BLOCK_TOKENS
    peer_count = lax.axis_size("view")
    capacity = max(1, 2 * slot_count // peer_count)
    block_count = tokens // BLOCK_TOKENS
    view_index = lax.axis_index("view")
    head_index = lax.axis_index("head")
    score_scale = HEAD_DIM ** (-0.5)
    slot_order = jnp.arange(slot_count, dtype=jnp.int32)
    same_view = source_view[:, :, None] == source_view[:, None, :]
    earlier = slot_order[None, :] < slot_order[:, None]
    slot_rank = jnp.sum((same_view & earlier[None]).astype(jnp.int32), axis=2)
    copy_order = jnp.arange(capacity, dtype=jnp.int32)
    matched = (source_view == view_index)[:, :, None] & (
        slot_rank[:, :, None] == copy_order[None, None, :]
    )
    filled = jnp.any(matched, axis=1)
    chosen = jnp.sum(jnp.where(matched, source_block[:, :, None], 0), axis=1)
    own_view = lax.dynamic_index_in_dim(source_view, view_index, 0, keepdims=False)
    own_rank = lax.dynamic_index_in_dim(slot_rank, view_index, 0, keepdims=False)
    landing = own_view * capacity + own_rank
    joined = jnp.concatenate([key_rows, value_rows], axis=1)
    outgoing = jnp.take(
        joined.reshape(block_count, BLOCK_TOKENS, 2 * columns), chosen.reshape(-1), axis=0
    )
    outgoing = outgoing.reshape(peer_count, capacity, BLOCK_TOKENS, 2 * columns)
    incoming = lax.all_to_all(outgoing, "view", split_axis=0, concat_axis=0, tiled=True)
    fetched = jnp.take(
        incoming.reshape(peer_count * capacity, BLOCK_TOKENS, 2 * columns), landing, axis=0
    )
    fetched = fetched.reshape(key_count, 2 * columns)
    query_block = min(512, tokens)
    block_total = tokens // query_block
    key_heads = fetched[:, :columns].reshape(key_count, heads_here, HEAD_DIM)
    value_heads = fetched[:, columns:].reshape(key_count, heads_here, HEAD_DIM)
    query_heads = query_rows.reshape(block_total, query_block, heads_here, HEAD_DIM)

    def forward_step(query_part):
        scores = score_rows(query_part, key_heads, score_scale)
        row_top = jnp.max(scores, axis=-1, keepdims=True)
        shifted = jnp.exp(scores - row_top)
        row_total = jnp.sum(shifted, axis=-1, keepdims=True)
        weights = (shifted / row_total).astype(jnp.bfloat16)
        out_part = jnp.einsum(
            "hqk,khd->qhd", weights, value_heads, preferred_element_type=jnp.float32
        )
        return (out_part.astype(jnp.bfloat16), row_top, row_total)

    attended, row_tops, row_totals = lax.map(forward_step, query_heads)
    attended_rows = attended.reshape(tokens, columns)
    own_rows = lax.dynamic_slice_in_dim(out_weight, head_index * columns, columns, 0)
    part_weight = own_rows
    summed_rows = lax.psum_scatter(
        lax.dot_general(
            part_weight, attended_rows, (((0,), (1,)), ((), ())), preferred_element_type=jnp.float32
        ).astype(jnp.bfloat16),
        "head",
        scatter_dimension=0,
        tiled=True,
    ).astype(jnp.float32)
    mixed_out = summed_rows.T.astype(jnp.bfloat16)
    part_weight = own_rows
    attended_grad = lax.dot_general(
        lax.all_gather(out_grad, "head", axis=1, tiled=True),
        part_weight,
        (((1,), (1,)), ((), ())),
        preferred_element_type=jnp.float32,
    )
    grad_heads = attended_grad.astype(jnp.bfloat16).reshape(
        block_total, query_block, heads_here, HEAD_DIM
    )

    def backward_step(totals, inputs):
        key_total, value_total = totals
        query_part, out_part, grad_part, row_top, row_total = inputs
        scores = score_rows(query_part, key_heads, score_scale)
        probability = jnp.exp(scores - row_top) / row_total
        weights = probability.astype(jnp.bfloat16)
        grad_prob = jnp.einsum(
            "qhd,khd->hqk", grad_part, value_heads, preferred_element_type=jnp.float32
        )
        row_delta = jnp.einsum(
            "qhd,qhd->hq", out_part, grad_part, preferred_element_type=jnp.float32
        )[:, :, None]
        grad_scores = (probability * (grad_prob - row_delta)).astype(jnp.bfloat16)
        query_part_grad = (
            jnp.einsum("hqk,khd->qhd", grad_scores, key_heads, preferred_element_type=jnp.float32)
            * score_scale
        )
        key_total = (
            key_total
            + jnp.einsum(
                "hqk,qhd->khd", grad_scores, query_part, preferred_element_type=jnp.float32
            )
            * score_scale
        )
        value_total = value_total + jnp.einsum(
            "hqk,qhd->khd", weights, grad_part, preferred_element_type=jnp.float32
        )
        return ((key_total, value_total), query_part_grad.astype(jnp.bfloat16))

    zero_keys = jnp.zeros((key_count, heads_here, HEAD_DIM), jnp.float32)
    (key_total, value_total), query_grads = lax.scan(
        backward_step,
        (zero_keys, zero_keys),
        (query_heads, attended, grad_heads, row_tops, row_totals),
    )
    query_grad = query_grads.reshape(tokens, columns)
    slot_grads = jnp.concatenate(
        [key_total.reshape(key_count, columns), value_total.reshape(key_count, columns)], axis=1
    )
    slot_grads = slot_grads.reshape(slot_count, BLOCK_TOKENS * 2 * columns)
    placing = (
        landing[None, :] == jnp.arange(peer_count * capacity, dtype=jnp.int32)[:, None]
    ).astype(jnp.float32)
    outgoing_grads = jnp.dot(placing, slot_grads, precision=lax.Precision.HIGHEST).reshape(
        peer_count, capacity, BLOCK_TOKENS, 2 * columns
    )
    returned = lax.all_to_all(
        outgoing_grads.astype(jnp.bfloat16), "view", split_axis=0, concat_axis=0, tiled=True
    ).astype(outgoing_grads.dtype)
    gathering = (
        chosen.reshape(-1)[None, :] == jnp.arange(block_count, dtype=jnp.int32)[:, None]
    ) & filled.reshape(-1)[None, :]
    summed = jnp.dot(
        gathering.astype(jnp.float32),
        returned.reshape(peer_count * capacity, BLOCK_TOKENS * 2 * columns),
        precision=lax.Precision.HIGHEST,
    )
    summed = summed.reshape(tokens, 2 * columns)
    key_grad = summed[:, :columns].astype(jnp.bfloat16)
    value_grad = summed[:, columns:].astype(jnp.bfloat16)
    return (mixed_out, query_grad, key_grad, value_grad)


def planes(*args):
    return plane_body(*args)


def solution(mesh):
    placed = P("view", "head")
    views, group = mesh.shape["view"], mesh.shape["head"]

    def step(*args):
        tokens, columns = args[0].shape
        count = columns // group // HEAD_DIM
        fits = (
            views == 2 * count
            and count > 1
            and count & (count - 1) == 0
            and group & (group - 1) == 0
            and tokens // views % (4 * BLOCK_TOKENS) == 0
        )
        inner = jax.shard_map(
            planes if fits else body,
            mesh=mesh,
            in_specs=(placed, placed, placed, P(), placed, P(), P()),
            out_specs=(placed,) * 4,
            check_vma=False,
        )
        return inner(*args)

    return step
```

```python
import jax
import jax.numpy as jnp
from jax import lax
from jax.experimental import pallas as pl
from jax.experimental.pallas import tpu as pltpu
from jax.sharding import PartitionSpec as P


HEAD_DIM = 64
BLOCK_TOKENS = 128
SCALE = HEAD_DIM**-0.5
LOG2E = 1.4426950408889634
F32 = jnp.float32
BF16 = jnp.bfloat16
HBM = pl.BlockSpec(memory_space=pl.ANY)
STEP = 256


def join(a, b):
    return jnp.concatenate([a[:, :HEAD_DIM], b[:, :HEAD_DIM]], axis=1)


def join_high(a, b):
    return jnp.concatenate([a[:, HEAD_DIM:], b[:, HEAD_DIM:]], axis=1)


def dot(a, b):
    return jnp.dot(a, b, preferred_element_type=F32)


def aligned(index, size):
    return pl.ds(pl.multiple_of(index * size, size), size)


def call(kernel, scalars, args, in_specs, out_specs, out_shape, grid=(1,), scratch=(), flops=0):
    return pl.pallas_call(
        kernel,
        grid_spec=pltpu.PrefetchScalarGridSpec(
            num_scalar_prefetch=len(scalars),
            grid=grid,
            in_specs=in_specs,
            out_specs=out_specs,
            scratch_shapes=list(scratch),
        ),
        out_shape=out_shape,
        compiler_params=pltpu.CompilerParams(dimension_semantics=("arbitrary",) * len(grid)),
        cost_estimate=pl.CostEstimate(flops=flops, transcendentals=0, bytes_accessed=0)
        if flops
        else None,
    )(*scalars, *args)


def whole(*shape):
    return pl.BlockSpec(shape, lambda *_: (0,) * len(shape))


def shape_of(*shape, dtype=BF16):
    return jax.ShapeDtypeStruct(shape, dtype)


def run_copies(*copies):
    for copy in copies:
        copy.start()
    for copy in copies:
        copy.wait()


def fold_pair(x_ref, out_ref):
    rows = out_ref.shape[2]
    top, low = x_ref[:rows, :], x_ref[rows:, :]
    for n in range(out_ref.shape[0]):
        out_ref[n, 0] = join(top, low)
        out_ref[n, 1] = join_high(top, low)


def fold_each(meta_ref, x_ref, outs):
    rows = x_ref.shape[0]
    count = x_ref.shape[1] // HEAD_DIM
    for n, out in enumerate(outs):
        head = meta_ref[0] ^ (n % count)
        pair = aligned(head // 2, 128)
        top, low = x_ref[: rows // 2, pair], x_ref[rows // 2 :, pair]
        out[...] = jnp.where(head % 2 == 1, join_high(top, low), join(top, low))


def pack_k(x_ref, out_ref):
    fold_pair(x_ref, out_ref)


def pack_v(meta_ref, x_ref, *outs):
    fold_each(meta_ref, x_ref, outs)


def pack_q(meta_ref, x_ref, *outs):
    fold_each(meta_ref, x_ref, outs)


def spread(parts, out_ref):
    rows = out_ref.shape[0] // 2
    for head in range(0, len(parts), 2):
        lanes = slice(HEAD_DIM * head, HEAD_DIM * (head + 2))
        out_ref[:rows, lanes] = join(parts[head], parts[head + 1])
        out_ref[rows:, lanes] = join_high(parts[head], parts[head + 1])


def collect(meta_ref, *refs):
    parts, (out_ref, scr, sem) = refs[:-3], refs[-3:]
    run_copies(
        *(
            pltpu.make_async_copy(part, scr.at[meta_ref[0] ^ n], sem.at[n])
            for n, part in enumerate(parts)
        )
    )
    spread([scr[n] for n in range(len(parts))], out_ref)


def total_pair(x_ref, out_ref):
    parts = []
    for head in range(2):
        part = x_ref[0, head].astype(F32)
        for n in range(1, x_ref.shape[0]):
            part = part + x_ref[n, head].astype(F32)
        parts.append(part.astype(BF16))
    spread(parts, out_ref)


def total_k(x_ref, out_ref):
    total_pair(x_ref, out_ref)


def total_v(x_ref, out_ref):
    total_pair(x_ref, out_ref)


def attended_grads(meta_ref, own_ref, *refs):
    count = own_ref.shape[1] // HEAD_DIM
    outs, scr = refs[-1 - count : -1], refs[-1]
    parts, w_ref = (own_ref, *refs[: -2 - count]), refs[-2 - count]
    columns = own_ref.shape[1]
    total = None
    for n, part in enumerate(parts):
        piece = lax.dot_general(
            part[...],
            w_ref[:, aligned(meta_ref[2] ^ n, columns)],
            (((1,), (1,)), ((), ())),
            preferred_element_type=F32,
        )
        total = piece if total is None else total + piece
    scr[...] = total.astype(BF16)
    fold_each(meta_ref, scr, outs)


def mix(meta_ref, *refs):
    parts, (w_ref, out_ref) = refs[:-2], refs[-2:]
    columns = out_ref.shape[1]
    total = None
    for n, part in enumerate(parts):
        piece = dot(part[...], w_ref[aligned(meta_ref[2] ^ n, columns), :])
        total = piece if total is None else total + piece
    out_ref[...] = total.astype(BF16)


def place(sv_ref, sb_ref, view, slot, per_half):
    block = sb_ref[view, slot]
    return sv_ref[view, slot], lax.div(block, per_half), aligned(lax.rem(block, per_half), BLOCK_TOKENS)


def gather(sv_ref, sb_ref, view, src, rows_scr=None, turned_scr=None):
    per_half = src.shape[1] // BLOCK_TOKENS
    for slot in range(sv_ref.shape[1]):
        source, high, rows = place(sv_ref, sb_ref, view, slot, per_half)
        block = src[source, rows, :]
        block = jnp.where(high == 1, join_high(block, block), block)
        span = slice(slot * BLOCK_TOKENS, (slot + 1) * BLOCK_TOKENS)
        if rows_scr is not None:
            rows_scr[span, :] = block
        if turned_scr is not None:
            turned_scr[:, span] = block.T[:HEAD_DIM]


def scatter(sv_ref, sb_ref, view, acc, lhs, rhs):
    per_view = acc.shape[1] // BLOCK_TOKENS
    keys = sv_ref.shape[1] * BLOCK_TOKENS
    for start in range(0, keys, STEP):
        part = None
        for a, b in zip(lhs, rhs):
            piece = dot(a[start : start + STEP, :], b)
            part = piece if part is None else part + piece
        for inner in range(0, STEP, BLOCK_TOKENS):
            source, _, rows = place(sv_ref, sb_ref, view, (start + inner) // BLOCK_TOKENS, per_view)
            acc[source, rows, :] += part[inner : inner + BLOCK_TOKENS]


def give_back(acc, out_ref):
    rows = out_ref.shape[1]
    for view in range(acc.shape[0]):
        block = acc[view].astype(BF16)
        out_ref[view] = join(block[:rows], block[rows:])


def halves(block):
    t = block.T
    return [t[:HEAD_DIM], t[HEAD_DIM:]]


def padded(t):
    return jnp.concatenate([t, jnp.zeros_like(t)], axis=0)


def view_copies(meta_ref, count, parts, scr, sems):
    here = meta_ref[1] * count + meta_ref[0]
    return [
        pltpu.make_async_copy(part, scr.at[here ^ n], sem)
        for n, (part, sem) in enumerate(zip(parts, sems))
    ]


def scores(sv_ref, sb_ref, meta_ref, k_ref, *refs):
    count = len(refs) - 8
    parts = refs[:count]
    e_ref, l_ref, k_scr, q_scr, rows_scr, s0, s1, sem = refs[count:]
    step = pl.program_id(0)

    @pl.when(step == 0)
    def _():
        run_copies(
            pltpu.make_async_copy(k_ref, k_scr, sem.at[count]),
            *(pltpu.make_async_copy(p, q_scr.at[n], sem.at[n]) for n, p in enumerate(parts)),
        )

    view = meta_ref[1] * count + (meta_ref[0] ^ step)
    gather(sv_ref, sb_ref, view, k_scr, rows_scr=rows_scr)
    keys, queries = s0.shape
    tops = []
    for t, s_scr in zip(halves(q_scr[step]), (s0, s1)):
        q = padded(t * jnp.asarray(SCALE, BF16))
        top = None
        for i in range(0, keys, STEP):
            s = dot(rows_scr[i : i + STEP, :], q)
            s_scr[i : i + STEP, :] = s
            m = jnp.max(s.reshape(STEP // 8, 8, queries), axis=0)
            top = m if top is None else jnp.maximum(top, m)
        tops.append(jnp.max(top, axis=0, keepdims=True))
    for n, (top, s_scr) in enumerate(zip(tops, (s0, s1))):
        total = None
        for i in range(0, keys, STEP):
            e = jnp.exp2((s_scr[i : i + STEP, :] - top) * LOG2E)
            m = jnp.sum(e.reshape(STEP // 8, 8, queries), axis=0)
            total = m if total is None else total + m
            e_ref[0, n, i : i + STEP, :] = e.astype(BF16)
        l_ref[0, n] = jnp.sum(total, axis=0, keepdims=True)


def attend(sv_ref, sb_ref, meta_ref, *refs):
    v_scr, g_scr, turned_scr, acc, sem = refs[-5:]
    count, views = g_scr.shape[0], v_scr.shape[0]
    v_parts, parts = refs[:views], refs[views : views + count]
    e_ref, l_ref = refs[views + count : views + count + 2]
    outs = refs[views + count + 2 : views + 2 * count + 2]
    delta_ref, dv_ref = refs[views + 2 * count + 2 : -5]
    step = pl.program_id(0)

    @pl.when(step == 0)
    def _():
        run_copies(
            *view_copies(meta_ref, count, v_parts, v_scr, [sem.at[count + n] for n in range(views)]),
            *(pltpu.make_async_copy(p, g_scr.at[n], sem.at[n]) for n, p in enumerate(parts)),
        )
        acc[...] = jnp.zeros_like(acc)

    view = meta_ref[1] * count + (meta_ref[0] ^ step)
    gather(sv_ref, sb_ref, view, v_scr, turned_scr=turned_scr)
    out, grads = [], []
    for n, g in enumerate(halves(g_scr[step])):
        o = (dot(turned_scr[...], e_ref[0, n]) / l_ref[0, n]).astype(BF16)
        g = (g.astype(F32) / l_ref[0, n]).astype(BF16)
        delta_ref[0, n] = jnp.sum(o.astype(F32) * g.astype(F32), axis=0, keepdims=True)
        out.append(o)
        grads.append(padded(g).T)
    out = jnp.concatenate(out, axis=0).T
    for n, ref in enumerate(outs):

        @pl.when(step == n)
        def _():
            ref[...] = out

    scatter(sv_ref, sb_ref, view, acc, (e_ref.at[0, 0], e_ref.at[0, 1]), grads)

    @pl.when(step == count - 1)
    def _():
        give_back(acc, dv_ref)


def backward(sv_ref, sb_ref, meta_ref, k_ref, *refs):
    k_scr, v_scr, q_scr, g_scr, rows_scr, turned_scr, ds0, ds1, acc, sem = refs[-10:]
    count, views = q_scr.shape[0], v_scr.shape[0]
    v_parts, refs = refs[:views], refs[views:]
    q_parts, g_parts = refs[:count], refs[count : 2 * count]
    e_ref, l_ref, delta_ref = refs[2 * count : 2 * count + 3]
    outs = refs[2 * count + 3 : 3 * count + 3]
    dk_ref = refs[3 * count + 3]
    step = pl.program_id(0)

    @pl.when(step == 0)
    def _():
        run_copies(
            pltpu.make_async_copy(k_ref, k_scr, sem.at[2 * count]),
            *view_copies(
                meta_ref, count, v_parts, v_scr, [sem.at[2 * count + 1 + n] for n in range(views)]
            ),
            *(pltpu.make_async_copy(p, q_scr.at[n], sem.at[n]) for n, p in enumerate(q_parts)),
            *(
                pltpu.make_async_copy(p, g_scr.at[n], sem.at[count + n])
                for n, p in enumerate(g_parts)
            ),
        )
        acc[...] = jnp.zeros_like(acc)

    view = meta_ref[1] * count + (meta_ref[0] ^ step)
    gather(sv_ref, sb_ref, view, v_scr, rows_scr=rows_scr)
    gather(sv_ref, sb_ref, view, k_scr, turned_scr=turned_scr)
    keys = rows_scr.shape[0]
    queries = [padded(t * jnp.asarray(SCALE, BF16)).T for t in halves(q_scr[step])]
    for n, (g, ds_scr) in enumerate(zip(halves(g_scr[step]), (ds0, ds1))):
        g = padded((g.astype(F32) / l_ref[0, n]).astype(BF16))
        for i in range(0, keys, STEP):
            dp = dot(rows_scr[i : i + STEP, :], g)
            e = e_ref[0, n, i : i + STEP, :].astype(F32)
            ds_scr[i : i + STEP, :] = (e * (dp - delta_ref[0, n])).astype(BF16)
    scatter(sv_ref, sb_ref, view, acc, (ds0, ds1), queries)
    dq = [(dot(turned_scr[...], ds[...]) * SCALE).astype(BF16) for ds in (ds0, ds1)]
    dq = jnp.concatenate(dq, axis=0).T
    for n, ref in enumerate(outs):

        @pl.when(step == n)
        def _():
            ref[...] = dq

    @pl.when(step == count - 1)
    def _():
        give_back(acc, dk_ref)


def plane_body(query_rows, key_rows, value_rows, out_weight, out_grad, source_view, source_block):
    tokens, columns = query_rows.shape
    half = tokens // 2
    count = columns // HEAD_DIM
    views = lax.axis_size("view")
    group = lax.axis_size("head")
    keys = source_view.shape[1] * BLOCK_TOKENS
    head_index = lax.axis_index("head").astype(jnp.int32)
    view_index = lax.axis_index("view").astype(jnp.int32)
    meta = jnp.stack([lax.rem(view_index, count), lax.div(view_index, count), head_index])
    routes = (source_view, source_block, meta)

    def flip(x, bits):
        return lax.ppermute(x, "head", [(n, n ^ bits) for n in range(group)])

    def gathered(x):
        parts = {0: x}
        bits = group // 2
        while bits:
            for n, part in list(parts.items()):
                parts[n + bits] = flip(part, bits)
            bits //= 2
        return [parts[n] for n in range(group)]

    def view_swap(x):
        return lax.all_to_all(x, "view", split_axis=0, concat_axis=0, tiled=True)

    def send(parts):
        return [parts[0]] + [
            lax.ppermute(part, "view", [(n, n ^ bits) for n in range(views)])
            for bits, part in enumerate(parts)
            if bits
        ]

    full, rows_shape = whole(tokens, columns), shape_of(tokens, columns)
    one, one_shape = whole(half, 128), shape_of(half, 128)
    every, every_shape = whole(views, half, 128), shape_of(views, half, 128)
    groups = views // count
    strip = pl.BlockSpec((tokens, 128), lambda i: (0, i))
    duo = pl.BlockSpec((groups, 2, half, 128), lambda i: (0, i, 0, 0))
    duo_shape = shape_of(groups, count, half, 128)

    def packed(kernel, x):
        out = call(kernel, (), (x,), [strip], duo, duo_shape, grid=(count // 2,))
        return out.reshape(views, half, 128)

    def totalled(kernel, x):
        x = x.reshape(groups, count, half, 128)
        return call(kernel, (), (x,), [duo], strip, rows_shape, grid=(count // 2,))

    k = packed(pack_k, key_rows)
    k = view_swap(k)
    q = call(pack_q, (meta,), (query_rows,), [full], [one] * count, [one_shape] * count)
    q = send(q)
    og = gathered(out_grad)
    v = call(pack_v, (meta,), (value_rows,), [full], [one] * views, [one_shape] * views)
    v = send(v)
    g = call(
        attended_grads,
        (meta,),
        (*og, out_weight),
        [full] * group + [pl.BlockSpec((columns, group * columns), lambda i, m: (m[2], 0))],
        [one] * count,
        [one_shape] * count,
        scratch=[pltpu.VMEM((tokens, columns), BF16)],
    )
    g = send(g)
    e_spec = pl.BlockSpec((1, 2, keys, half), lambda i, *_: (i, 0, 0, 0))
    row_spec = pl.BlockSpec((1, 2, 1, half), lambda i, *_: (i, 0, 0, 0))
    row_shape = shape_of(count, 2, 1, half, dtype=F32)
    unit = 2 * count * keys * tokens * HEAD_DIM
    held = pltpu.VMEM((views, half, 128), BF16)
    mine = pltpu.VMEM((count, half, 128), BF16)
    totals = pltpu.VMEM((views, tokens, 128), F32)
    rows_scr = pltpu.VMEM((keys, 128), BF16)
    turned_scr = pltpu.VMEM((HEAD_DIM, keys), BF16)
    e, l = call(
        scores,
        routes,
        (k, *q),
        [HBM] * (1 + count),
        [e_spec, row_spec],
        [shape_of(count, 2, keys, half), row_shape],
        grid=(count,),
        scratch=[
            held, mine, rows_scr, pltpu.VMEM((keys, half), F32), pltpu.VMEM((keys, half), F32),
            pltpu.SemaphoreType.DMA((count + 1,)),
        ],
        flops=unit * 4,
    )
    *o, delta, dv = call(
        attend,
        routes,
        (*v, *g, e, l),
        [HBM] * (views + count) + [e_spec, row_spec],
        [one] * count + [row_spec, every],
        [one_shape] * count + [row_shape, every_shape],
        grid=(count,),
        scratch=[held, mine, turned_scr, totals, pltpu.SemaphoreType.DMA((count + views,))],
        flops=unit * 3,
    )
    dv = view_swap(dv)
    o = send(o)
    *dq, dk = call(
        backward,
        routes,
        (k, *v, *q, *g, e, l, delta),
        [HBM] * (1 + views + 2 * count) + [e_spec, row_spec, row_spec],
        [one] * count + [every],
        [one_shape] * count + [every_shape],
        grid=(count,),
        scratch=[
            held, held, mine, mine, rows_scr, turned_scr,
            pltpu.VMEM((keys, half), BF16), pltpu.VMEM((keys, half), BF16),
            totals, pltpu.SemaphoreType.DMA((2 * count + 1 + views,)),
        ],
        flops=unit * 8,
    )
    dk = view_swap(dk)
    dq = send(dq)

    def collected(parts):
        return call(
            collect, (meta,), tuple(parts), [HBM] * count, full, rows_shape,
            scratch=[mine, pltpu.SemaphoreType.DMA((count,))],
        )

    attended = collected(o)
    attended = gathered(attended)
    mixed_out = call(
        mix,
        (meta,),
        (*attended, out_weight),
        [full] * group + [pl.BlockSpec((group * columns, columns), lambda i, m: (0, m[2]))],
        full,
        rows_shape,
    )
    value_grad = totalled(total_v, dv)
    query_grad = collected(dq)
    key_grad = totalled(total_k, dk)
    return mixed_out, query_grad, key_grad, value_grad


def score_rows(query_part, key_heads, score_scale):
    return (
        jnp.einsum("qhd,khd->hqk", query_part, key_heads, preferred_element_type=jnp.float32)
        * score_scale
    )


def body(query_rows, key_rows, value_rows, out_weight, out_grad, source_view, source_block):
    tokens = query_rows.shape[0]
    columns = query_rows.shape[1]
    heads_here = columns // HEAD_DIM
    slot_count = source_view.shape[1]
    key_count = slot_count * BLOCK_TOKENS
    peer_count = lax.axis_size("view")
    capacity = max(1, 2 * slot_count // peer_count)
    block_count = tokens // BLOCK_TOKENS
    view_index = lax.axis_index("view")
    head_index = lax.axis_index("head")
    score_scale = HEAD_DIM ** (-0.5)
    slot_order = jnp.arange(slot_count, dtype=jnp.int32)
    same_view = source_view[:, :, None] == source_view[:, None, :]
    earlier = slot_order[None, :] < slot_order[:, None]
    slot_rank = jnp.sum((same_view & earlier[None]).astype(jnp.int32), axis=2)
    copy_order = jnp.arange(capacity, dtype=jnp.int32)
    matched = (source_view == view_index)[:, :, None] & (
        slot_rank[:, :, None] == copy_order[None, None, :]
    )
    filled = jnp.any(matched, axis=1)
    chosen = jnp.sum(jnp.where(matched, source_block[:, :, None], 0), axis=1)
    own_view = lax.dynamic_index_in_dim(source_view, view_index, 0, keepdims=False)
    own_rank = lax.dynamic_index_in_dim(slot_rank, view_index, 0, keepdims=False)
    landing = own_view * capacity + own_rank
    joined = jnp.concatenate([key_rows, value_rows], axis=1)
    outgoing = jnp.take(
        joined.reshape(block_count, BLOCK_TOKENS, 2 * columns), chosen.reshape(-1), axis=0
    )
    outgoing = outgoing.reshape(peer_count, capacity, BLOCK_TOKENS, 2 * columns)
    incoming = lax.all_to_all(outgoing, "view", split_axis=0, concat_axis=0, tiled=True)
    fetched = jnp.take(
        incoming.reshape(peer_count * capacity, BLOCK_TOKENS, 2 * columns), landing, axis=0
    )
    fetched = fetched.reshape(key_count, 2 * columns)
    query_block = min(512, tokens)
    block_total = tokens // query_block
    key_heads = fetched[:, :columns].reshape(key_count, heads_here, HEAD_DIM)
    value_heads = fetched[:, columns:].reshape(key_count, heads_here, HEAD_DIM)
    query_heads = query_rows.reshape(block_total, query_block, heads_here, HEAD_DIM)

    def forward_step(query_part):
        scores = score_rows(query_part, key_heads, score_scale)
        row_top = jnp.max(scores, axis=-1, keepdims=True)
        shifted = jnp.exp(scores - row_top)
        row_total = jnp.sum(shifted, axis=-1, keepdims=True)
        weights = (shifted / row_total).astype(jnp.bfloat16)
        out_part = jnp.einsum(
            "hqk,khd->qhd", weights, value_heads, preferred_element_type=jnp.float32
        )
        return (out_part.astype(jnp.bfloat16), row_top, row_total)

    attended, row_tops, row_totals = lax.map(forward_step, query_heads)
    attended_rows = attended.reshape(tokens, columns)
    own_rows = lax.dynamic_slice_in_dim(out_weight, head_index * columns, columns, 0)
    part_weight = own_rows
    summed_rows = lax.psum_scatter(
        lax.dot_general(
            part_weight, attended_rows, (((0,), (1,)), ((), ())), preferred_element_type=jnp.float32
        ).astype(jnp.bfloat16),
        "head",
        scatter_dimension=0,
        tiled=True,
    ).astype(jnp.float32)
    mixed_out = summed_rows.T.astype(jnp.bfloat16)
    part_weight = own_rows
    attended_grad = lax.dot_general(
        lax.all_gather(out_grad, "head", axis=1, tiled=True),
        part_weight,
        (((1,), (1,)), ((), ())),
        preferred_element_type=jnp.float32,
    )
    grad_heads = attended_grad.astype(jnp.bfloat16).reshape(
        block_total, query_block, heads_here, HEAD_DIM
    )

    def backward_step(totals, inputs):
        key_total, value_total = totals
        query_part, out_part, grad_part, row_top, row_total = inputs
        scores = score_rows(query_part, key_heads, score_scale)
        probability = jnp.exp(scores - row_top) / row_total
        weights = probability.astype(jnp.bfloat16)
        grad_prob = jnp.einsum(
            "qhd,khd->hqk", grad_part, value_heads, preferred_element_type=jnp.float32
        )
        row_delta = jnp.einsum(
            "qhd,qhd->hq", out_part, grad_part, preferred_element_type=jnp.float32
        )[:, :, None]
        grad_scores = (probability * (grad_prob - row_delta)).astype(jnp.bfloat16)
        query_part_grad = (
            jnp.einsum("hqk,khd->qhd", grad_scores, key_heads, preferred_element_type=jnp.float32)
            * score_scale
        )
        key_total = (
            key_total
            + jnp.einsum(
                "hqk,qhd->khd", grad_scores, query_part, preferred_element_type=jnp.float32
            )
            * score_scale
        )
        value_total = value_total + jnp.einsum(
            "hqk,qhd->khd", weights, grad_part, preferred_element_type=jnp.float32
        )
        return ((key_total, value_total), query_part_grad.astype(jnp.bfloat16))

    zero_keys = jnp.zeros((key_count, heads_here, HEAD_DIM), jnp.float32)
    (key_total, value_total), query_grads = lax.scan(
        backward_step,
        (zero_keys, zero_keys),
        (query_heads, attended, grad_heads, row_tops, row_totals),
    )
    query_grad = query_grads.reshape(tokens, columns)
    slot_grads = jnp.concatenate(
        [key_total.reshape(key_count, columns), value_total.reshape(key_count, columns)], axis=1
    )
    slot_grads = slot_grads.reshape(slot_count, BLOCK_TOKENS * 2 * columns)
    placing = (
        landing[None, :] == jnp.arange(peer_count * capacity, dtype=jnp.int32)[:, None]
    ).astype(jnp.float32)
    outgoing_grads = jnp.dot(placing, slot_grads, precision=lax.Precision.HIGHEST).reshape(
        peer_count, capacity, BLOCK_TOKENS, 2 * columns
    )
    returned = lax.all_to_all(
        outgoing_grads.astype(jnp.bfloat16), "view", split_axis=0, concat_axis=0, tiled=True
    ).astype(outgoing_grads.dtype)
    gathering = (
        chosen.reshape(-1)[None, :] == jnp.arange(block_count, dtype=jnp.int32)[:, None]
    ) & filled.reshape(-1)[None, :]
    summed = jnp.dot(
        gathering.astype(jnp.float32),
        returned.reshape(peer_count * capacity, BLOCK_TOKENS * 2 * columns),
        precision=lax.Precision.HIGHEST,
    )
    summed = summed.reshape(tokens, 2 * columns)
    key_grad = summed[:, :columns].astype(jnp.bfloat16)
    value_grad = summed[:, columns:].astype(jnp.bfloat16)
    return (mixed_out, query_grad, key_grad, value_grad)


def planes(*args):
    return plane_body(*args)


def solution(mesh):
    placed = P("view", "head")
    views, group = mesh.shape["view"], mesh.shape["head"]

    def step(*args):
        tokens, columns = args[0].shape
        count = columns // group // HEAD_DIM
        fits = (
            views == 2 * count
            and count > 1
            and count & (count - 1) == 0
            and group & (group - 1) == 0
            and tokens // views % (4 * BLOCK_TOKENS) == 0
        )
        inner = jax.shard_map(
            planes if fits else body,
            mesh=mesh,
            in_specs=(placed, placed, placed, P(), placed, P(), P()),
            out_specs=(placed,) * 4,
            check_vma=False,
        )
        return inner(*args)

    return step
```

```python
import jax
import jax.numpy as jnp
from jax import lax
from jax.experimental import pallas as pl
from jax.experimental.pallas import tpu as pltpu
from jax.sharding import PartitionSpec as P


HEAD_DIM = 64
BLOCK_TOKENS = 128
SCALE = HEAD_DIM**-0.5
LOG2E = 1.4426950408889634
F32 = jnp.float32
BF16 = jnp.bfloat16
HBM = pl.BlockSpec(memory_space=pl.ANY)
STEP = 256


def join(a, b):
    return jnp.concatenate([a[:, :HEAD_DIM], b[:, :HEAD_DIM]], axis=1)


def join_high(a, b):
    return jnp.concatenate([a[:, HEAD_DIM:], b[:, HEAD_DIM:]], axis=1)


def dot(a, b):
    return jnp.dot(a, b, preferred_element_type=F32)


def aligned(index, size):
    return pl.ds(pl.multiple_of(index * size, size), size)


def call(kernel, scalars, args, in_specs, out_specs, out_shape, grid=(1,), scratch=(), flops=0):
    return pl.pallas_call(
        kernel,
        grid_spec=pltpu.PrefetchScalarGridSpec(
            num_scalar_prefetch=len(scalars),
            grid=grid,
            in_specs=in_specs,
            out_specs=out_specs,
            scratch_shapes=list(scratch),
        ),
        out_shape=out_shape,
        compiler_params=pltpu.CompilerParams(dimension_semantics=("arbitrary",) * len(grid)),
        cost_estimate=pl.CostEstimate(flops=flops, transcendentals=0, bytes_accessed=0)
        if flops
        else None,
    )(*scalars, *args)


def whole(*shape):
    return pl.BlockSpec(shape, lambda *_: (0,) * len(shape))


def shape_of(*shape, dtype=BF16):
    return jax.ShapeDtypeStruct(shape, dtype)


def run_copies(*copies):
    for copy in copies:
        copy.start()
    for copy in copies:
        copy.wait()


def fold_pair(x_ref, out_ref):
    rows = out_ref.shape[2]
    top, low = x_ref[:rows, :], x_ref[rows:, :]
    for n in range(out_ref.shape[0]):
        out_ref[n, 0] = join(top, low)
        out_ref[n, 1] = join_high(top, low)


def fold_each(meta_ref, x_ref, outs):
    rows = x_ref.shape[0]
    count = x_ref.shape[1] // HEAD_DIM
    for n, out in enumerate(outs):
        head = meta_ref[0] ^ (n % count)
        pair = aligned(head // 2, 128)
        top, low = x_ref[: rows // 2, pair], x_ref[rows // 2 :, pair]
        out[...] = jnp.where(head % 2 == 1, join_high(top, low), join(top, low))


def pack_k(x_ref, out_ref):
    fold_pair(x_ref, out_ref)


def pack_v(meta_ref, x_ref, *outs):
    fold_each(meta_ref, x_ref, outs)


def pack_q(meta_ref, x_ref, *outs):
    fold_each(meta_ref, x_ref, outs)


def spread(parts, out_ref):
    rows = out_ref.shape[0] // 2
    for head in range(0, len(parts), 2):
        lanes = slice(HEAD_DIM * head, HEAD_DIM * (head + 2))
        out_ref[:rows, lanes] = join(parts[head], parts[head + 1])
        out_ref[rows:, lanes] = join_high(parts[head], parts[head + 1])


def collect(meta_ref, *refs):
    parts, (out_ref, scr, sem) = refs[:-3], refs[-3:]
    run_copies(
        *(
            pltpu.make_async_copy(part, scr.at[meta_ref[0] ^ n], sem.at[n])
            for n, part in enumerate(parts)
        )
    )
    spread([scr[n] for n in range(len(parts))], out_ref)


def total_pair(x_ref, out_ref):
    parts = []
    for head in range(2):
        part = x_ref[0, head].astype(F32)
        for n in range(1, x_ref.shape[0]):
            part = part + x_ref[n, head].astype(F32)
        parts.append(part.astype(BF16))
    spread(parts, out_ref)


def total_k(x_ref, out_ref):
    total_pair(x_ref, out_ref)


def total_v(x_ref, out_ref):
    total_pair(x_ref, out_ref)


def attended_grads(meta_ref, own_ref, *refs):
    count = own_ref.shape[1] // HEAD_DIM
    outs, scr = refs[-1 - count : -1], refs[-1]
    parts, w_ref = (own_ref, *refs[: -2 - count]), refs[-2 - count]
    columns = own_ref.shape[1]
    total = None
    for n, part in enumerate(parts):
        piece = lax.dot_general(
            part[...],
            w_ref[:, aligned(meta_ref[2] ^ n, columns)],
            (((1,), (1,)), ((), ())),
            preferred_element_type=F32,
        )
        total = piece if total is None else total + piece
    scr[...] = total.astype(BF16)
    fold_each(meta_ref, scr, outs)


def mix(meta_ref, *refs):
    parts, (w_ref, out_ref) = refs[:-2], refs[-2:]
    columns = out_ref.shape[1]
    total = None
    for n, part in enumerate(parts):
        piece = dot(part[...], w_ref[aligned(meta_ref[2] ^ n, columns), :])
        total = piece if total is None else total + piece
    out_ref[...] = total.astype(BF16)


def place(sv_ref, sb_ref, view, slot, per_half):
    block = sb_ref[view, slot]
    return sv_ref[view, slot], lax.div(block, per_half), aligned(lax.rem(block, per_half), BLOCK_TOKENS)


def gather(sv_ref, sb_ref, view, src, rows_scr=None, turned_scr=None):
    per_half = src.shape[1] // BLOCK_TOKENS
    for slot in range(sv_ref.shape[1]):
        source, high, rows = place(sv_ref, sb_ref, view, slot, per_half)
        block = src[source, rows, :]
        block = jnp.where(high == 1, join_high(block, block), block)
        span = slice(slot * BLOCK_TOKENS, (slot + 1) * BLOCK_TOKENS)
        if rows_scr is not None:
            rows_scr[span, :] = block
        if turned_scr is not None:
            turned_scr[:, span] = block.T[:HEAD_DIM]


def scatter(sv_ref, sb_ref, view, acc, lhs, rhs):
    per_view = acc.shape[1] // BLOCK_TOKENS
    keys = sv_ref.shape[1] * BLOCK_TOKENS
    for start in range(0, keys, STEP):
        part = None
        for a, b in zip(lhs, rhs):
            piece = dot(a[start : start + STEP, :], b)
            part = piece if part is None else part + piece
        for inner in range(0, STEP, BLOCK_TOKENS):
            source, _, rows = place(sv_ref, sb_ref, view, (start + inner) // BLOCK_TOKENS, per_view)
            acc[source, rows, :] += part[inner : inner + BLOCK_TOKENS]


def give_back(acc, out_ref):
    rows = out_ref.shape[1]
    for view in range(acc.shape[0]):
        block = acc[view].astype(BF16)
        out_ref[view] = join(block[:rows], block[rows:])


def halves(block):
    t = block.T
    return [t[:HEAD_DIM], t[HEAD_DIM:]]


def padded(t):
    return jnp.concatenate([t, jnp.zeros_like(t)], axis=0)


def view_copies(meta_ref, count, parts, scr, sems):
    here = meta_ref[1] * count + meta_ref[0]
    return [
        pltpu.make_async_copy(part, scr.at[here ^ n], sem)
        for n, (part, sem) in enumerate(zip(parts, sems))
    ]


def scores(sv_ref, sb_ref, meta_ref, k_ref, *refs):
    e_ref, l_ref, k_scr, q_scr, rows_scr, top_scr, s0, s1, sem = refs[-9:]
    parts = refs[:-9]
    count = len(parts)
    step = pl.program_id(0)
    keys, queries = s0.shape
    chunk = 128

    @pl.when(step == 0)
    def _():
        run_copies(
            pltpu.make_async_copy(k_ref, k_scr, sem.at[count]),
            *(pltpu.make_async_copy(p, q_scr.at[n], sem.at[n]) for n, p in enumerate(parts)),
        )

    def phase(old, new, q, n):
        top = None
        total = None
        old_top = top_scr[...]
        for i in range(0, keys, chunk):
            rows = slice(i, i + chunk)
            if q is not None:
                s = dot(rows_scr[rows, :], q)
                new[rows, :] = s
                m = jnp.max(s.reshape(chunk // 8, 8, queries), axis=0)
                top = m if top is None else jnp.maximum(top, m)
            e = jnp.exp2((old[rows, :] - old_top) * LOG2E)
            m = jnp.sum(e.reshape(chunk // 8, 8, queries), axis=0)
            total = m if total is None else total + m
            e_ref[0, n, rows, :] = e.astype(BF16)
        l_ref[0, n] = jnp.sum(total, axis=0, keepdims=True)
        if q is not None:
            top_scr[...] = jnp.max(top, axis=0, keepdims=True)

    @pl.when(step < count)
    def _():
        view = meta_ref[1] * count + (meta_ref[0] ^ step)
        gather(sv_ref, sb_ref, view, k_scr, rows_scr=rows_scr)
        first, second = [padded(t * jnp.asarray(SCALE, BF16)) for t in halves(q_scr[step])]
        phase(s1, s0, first, 0)
        phase(s0, s1, second, 1)

    @pl.when(step == count)
    def _():
        phase(s1, None, None, 0)


def attend(sv_ref, sb_ref, meta_ref, *refs):
    v_scr, g_scr, turned_scr, acc, sem = refs[-5:]
    count, views = g_scr.shape[0], v_scr.shape[0]
    v_parts, parts = refs[:views], refs[views : views + count]
    e_refs = refs[views + count : views + count + 2]
    l_refs = refs[views + count + 2 : views + count + 4]
    outs = refs[views + count + 4 : views + 2 * count + 4]
    delta_ref, dv_ref = refs[views + 2 * count + 4 : -5]
    step = pl.program_id(0)

    @pl.when(step == 0)
    def _():
        run_copies(
            *view_copies(meta_ref, count, v_parts, v_scr, [sem.at[count + n] for n in range(views)]),
            *(pltpu.make_async_copy(p, g_scr.at[n], sem.at[n]) for n, p in enumerate(parts)),
        )
        acc[...] = jnp.zeros_like(acc)

    view = meta_ref[1] * count + (meta_ref[0] ^ step)
    gather(sv_ref, sb_ref, view, v_scr, turned_scr=turned_scr)
    out, grads = [], []
    for n, g in enumerate(halves(g_scr[step])):
        l = l_refs[n][0, 0]
        o = (dot(turned_scr[...], e_refs[n][0, 0]) / l).astype(BF16)
        g = (g.astype(F32) / l).astype(BF16)
        delta_ref[0, n] = jnp.sum(o.astype(F32) * g.astype(F32), axis=0, keepdims=True)
        out.append(o)
        grads.append(padded(g).T)
    out = jnp.concatenate(out, axis=0).T
    for n, ref in enumerate(outs):

        @pl.when(step == n)
        def _():
            ref[...] = out

    scatter(sv_ref, sb_ref, view, acc, [e.at[0, 0] for e in e_refs], grads)

    @pl.when(step == count - 1)
    def _():
        give_back(acc, dv_ref)


def backward(sv_ref, sb_ref, meta_ref, k_ref, *refs):
    k_scr, v_scr, q_scr, g_scr, rows_scr, turned_scr, ds0, ds1, acc, sem = refs[-10:]
    count, views = q_scr.shape[0], v_scr.shape[0]
    v_parts, refs = refs[:views], refs[views:]
    q_parts, g_parts = refs[:count], refs[count : 2 * count]
    e_refs, l_refs = refs[2 * count : 2 * count + 2], refs[2 * count + 2 : 2 * count + 4]
    delta_ref = refs[2 * count + 4]
    outs = refs[2 * count + 5 : 3 * count + 5]
    dk_ref = refs[3 * count + 5]
    step = pl.program_id(0)

    @pl.when(step == 0)
    def _():
        run_copies(
            pltpu.make_async_copy(k_ref, k_scr, sem.at[2 * count]),
            *view_copies(
                meta_ref, count, v_parts, v_scr, [sem.at[2 * count + 1 + n] for n in range(views)]
            ),
            *(pltpu.make_async_copy(p, q_scr.at[n], sem.at[n]) for n, p in enumerate(q_parts)),
            *(
                pltpu.make_async_copy(p, g_scr.at[n], sem.at[count + n])
                for n, p in enumerate(g_parts)
            ),
        )
        acc[...] = jnp.zeros_like(acc)

    view = meta_ref[1] * count + (meta_ref[0] ^ step)
    gather(sv_ref, sb_ref, view, v_scr, rows_scr=rows_scr)
    gather(sv_ref, sb_ref, view, k_scr, turned_scr=turned_scr)
    keys = rows_scr.shape[0]
    queries = [padded(t * jnp.asarray(SCALE, BF16)).T for t in halves(q_scr[step])]
    for n, (g, ds_scr) in enumerate(zip(halves(g_scr[step]), (ds0, ds1))):
        g = padded((g.astype(F32) / l_refs[n][0, 0]).astype(BF16))
        for i in range(0, keys, STEP):
            dp = dot(rows_scr[i : i + STEP, :], g)
            e = e_refs[n][0, 0, i : i + STEP, :].astype(F32)
            ds_scr[i : i + STEP, :] = (e * (dp - delta_ref[0, n])).astype(BF16)
    scatter(sv_ref, sb_ref, view, acc, (ds0, ds1), queries)
    dq = [(dot(turned_scr[...], ds[...]) * SCALE).astype(BF16) for ds in (ds0, ds1)]
    dq = jnp.concatenate(dq, axis=0).T
    for n, ref in enumerate(outs):

        @pl.when(step == n)
        def _():
            ref[...] = dq

    @pl.when(step == count - 1)
    def _():
        give_back(acc, dk_ref)


def plane_body(query_rows, key_rows, value_rows, out_weight, out_grad, source_view, source_block):
    tokens, columns = query_rows.shape
    half = tokens // 2
    count = columns // HEAD_DIM
    views = lax.axis_size("view")
    group = lax.axis_size("head")
    keys = source_view.shape[1] * BLOCK_TOKENS
    head_index = lax.axis_index("head").astype(jnp.int32)
    view_index = lax.axis_index("view").astype(jnp.int32)
    meta = jnp.stack([lax.rem(view_index, count), lax.div(view_index, count), head_index])
    routes = (source_view, source_block, meta)

    def flip(x, bits):
        return lax.ppermute(x, "head", [(n, n ^ bits) for n in range(group)])

    def gathered(x):
        parts = {0: x}
        bits = group // 2
        while bits:
            for n, part in list(parts.items()):
                parts[n + bits] = flip(part, bits)
            bits //= 2
        return [parts[n] for n in range(group)]

    def view_swap(x):
        return lax.all_to_all(x, "view", split_axis=0, concat_axis=0, tiled=True)

    def send(parts):
        return [parts[0]] + [
            lax.ppermute(part, "view", [(n, n ^ bits) for n in range(views)])
            for bits, part in enumerate(parts)
            if bits
        ]

    full, rows_shape = whole(tokens, columns), shape_of(tokens, columns)
    one, one_shape = whole(half, 128), shape_of(half, 128)
    every, every_shape = whole(views, half, 128), shape_of(views, half, 128)
    groups = views // count
    strip = pl.BlockSpec((tokens, 128), lambda i: (0, i))
    duo = pl.BlockSpec((groups, 2, half, 128), lambda i: (0, i, 0, 0))
    duo_shape = shape_of(groups, count, half, 128)

    def packed(kernel, x):
        out = call(kernel, (), (x,), [strip], duo, duo_shape, grid=(count // 2,))
        return out.reshape(views, half, 128)

    def totalled(kernel, x):
        x = x.reshape(groups, count, half, 128)
        return call(kernel, (), (x,), [duo], strip, rows_shape, grid=(count // 2,))

    k = packed(pack_k, key_rows)
    k = view_swap(k)
    q = call(pack_q, (meta,), (query_rows,), [full], [one] * count, [one_shape] * count)
    q = send(q)
    og = gathered(out_grad)
    v = call(pack_v, (meta,), (value_rows,), [full], [one] * views, [one_shape] * views)
    v = send(v)
    g = call(
        attended_grads,
        (meta,),
        (*og, out_weight),
        [full] * group + [pl.BlockSpec((columns, group * columns), lambda i, m: (m[2], 0))],
        [one] * count,
        [one_shape] * count,
        scratch=[pltpu.VMEM((tokens, columns), BF16)],
    )
    g = send(g)
    e_spec = pl.BlockSpec((1, 2, keys, half), lambda i, *_: (i, 0, 0, 0))
    e_specs = [
        pl.BlockSpec((1, 1, keys, half), lambda i, *_: (i, 1, 0, 0)),
        pl.BlockSpec((1, 1, keys, half), lambda i, *_: (i + 1, 0, 0, 0)),
    ]
    l_specs = [
        pl.BlockSpec((1, 1, 1, half), lambda i, *_: (i, 1, 0, 0)),
        pl.BlockSpec((1, 1, 1, half), lambda i, *_: (i + 1, 0, 0, 0)),
    ]
    row_spec = pl.BlockSpec((1, 2, 1, half), lambda i, *_: (i, 0, 0, 0))
    row_shape = shape_of(count, 2, 1, half, dtype=F32)
    unit = 2 * count * keys * tokens * HEAD_DIM
    held = pltpu.VMEM((views, half, 128), BF16)
    mine = pltpu.VMEM((count, half, 128), BF16)
    totals = pltpu.VMEM((views, tokens, 128), F32)
    rows_scr = pltpu.VMEM((keys, 128), BF16)
    turned_scr = pltpu.VMEM((HEAD_DIM, keys), BF16)
    e, l = call(
        scores,
        routes,
        (k, *q),
        [HBM] * (1 + count),
        [e_spec, row_spec],
        [shape_of(count + 1, 2, keys, half), shape_of(count + 1, 2, 1, half, dtype=F32)],
        grid=(count + 1,),
        scratch=[
            held, mine, rows_scr, pltpu.VMEM((1, half), F32), pltpu.VMEM((keys, half), F32), pltpu.VMEM((keys, half), F32),
            pltpu.SemaphoreType.DMA((count + 1,)),
        ],
        flops=unit * 4,
    )
    *o, delta, dv = call(
        attend,
        routes,
        (*v, *g, e, e, l, l),
        [HBM] * (views + count) + e_specs + l_specs,
        [one] * count + [row_spec, every],
        [one_shape] * count + [row_shape, every_shape],
        grid=(count,),
        scratch=[held, mine, turned_scr, totals, pltpu.SemaphoreType.DMA((count + views,))],
        flops=unit * 3,
    )
    dv = view_swap(dv)
    o = send(o)
    *dq, dk = call(
        backward,
        routes,
        (k, *v, *q, *g, e, e, l, l, delta),
        [HBM] * (1 + views + 2 * count) + e_specs + l_specs + [row_spec],
        [one] * count + [every],
        [one_shape] * count + [every_shape],
        grid=(count,),
        scratch=[
            held, held, mine, mine, rows_scr, turned_scr,
            pltpu.VMEM((keys, half), BF16), pltpu.VMEM((keys, half), BF16),
            totals, pltpu.SemaphoreType.DMA((2 * count + 1 + views,)),
        ],
        flops=unit * 8,
    )
    dk = view_swap(dk)
    dq = send(dq)

    def collected(parts):
        return call(
            collect, (meta,), tuple(parts), [HBM] * count, full, rows_shape,
            scratch=[mine, pltpu.SemaphoreType.DMA((count,))],
        )

    attended = collected(o)
    attended = gathered(attended)
    mixed_out = call(
        mix,
        (meta,),
        (*attended, out_weight),
        [full] * group + [pl.BlockSpec((group * columns, columns), lambda i, m: (0, m[2]))],
        full,
        rows_shape,
    )
    value_grad = totalled(total_v, dv)
    query_grad = collected(dq)
    key_grad = totalled(total_k, dk)
    return mixed_out, query_grad, key_grad, value_grad


def score_rows(query_part, key_heads, score_scale):
    return (
        jnp.einsum("qhd,khd->hqk", query_part, key_heads, preferred_element_type=jnp.float32)
        * score_scale
    )


def body(query_rows, key_rows, value_rows, out_weight, out_grad, source_view, source_block):
    tokens = query_rows.shape[0]
    columns = query_rows.shape[1]
    heads_here = columns // HEAD_DIM
    slot_count = source_view.shape[1]
    key_count = slot_count * BLOCK_TOKENS
    peer_count = lax.axis_size("view")
    capacity = max(1, 2 * slot_count // peer_count)
    block_count = tokens // BLOCK_TOKENS
    view_index = lax.axis_index("view")
    head_index = lax.axis_index("head")
    score_scale = HEAD_DIM ** (-0.5)
    slot_order = jnp.arange(slot_count, dtype=jnp.int32)
    same_view = source_view[:, :, None] == source_view[:, None, :]
    earlier = slot_order[None, :] < slot_order[:, None]
    slot_rank = jnp.sum((same_view & earlier[None]).astype(jnp.int32), axis=2)
    copy_order = jnp.arange(capacity, dtype=jnp.int32)
    matched = (source_view == view_index)[:, :, None] & (
        slot_rank[:, :, None] == copy_order[None, None, :]
    )
    filled = jnp.any(matched, axis=1)
    chosen = jnp.sum(jnp.where(matched, source_block[:, :, None], 0), axis=1)
    own_view = lax.dynamic_index_in_dim(source_view, view_index, 0, keepdims=False)
    own_rank = lax.dynamic_index_in_dim(slot_rank, view_index, 0, keepdims=False)
    landing = own_view * capacity + own_rank
    joined = jnp.concatenate([key_rows, value_rows], axis=1)
    outgoing = jnp.take(
        joined.reshape(block_count, BLOCK_TOKENS, 2 * columns), chosen.reshape(-1), axis=0
    )
    outgoing = outgoing.reshape(peer_count, capacity, BLOCK_TOKENS, 2 * columns)
    incoming = lax.all_to_all(outgoing, "view", split_axis=0, concat_axis=0, tiled=True)
    fetched = jnp.take(
        incoming.reshape(peer_count * capacity, BLOCK_TOKENS, 2 * columns), landing, axis=0
    )
    fetched = fetched.reshape(key_count, 2 * columns)
    query_block = min(512, tokens)
    block_total = tokens // query_block
    key_heads = fetched[:, :columns].reshape(key_count, heads_here, HEAD_DIM)
    value_heads = fetched[:, columns:].reshape(key_count, heads_here, HEAD_DIM)
    query_heads = query_rows.reshape(block_total, query_block, heads_here, HEAD_DIM)

    def forward_step(query_part):
        scores = score_rows(query_part, key_heads, score_scale)
        row_top = jnp.max(scores, axis=-1, keepdims=True)
        shifted = jnp.exp(scores - row_top)
        row_total = jnp.sum(shifted, axis=-1, keepdims=True)
        weights = (shifted / row_total).astype(jnp.bfloat16)
        out_part = jnp.einsum(
            "hqk,khd->qhd", weights, value_heads, preferred_element_type=jnp.float32
        )
        return (out_part.astype(jnp.bfloat16), row_top, row_total)

    attended, row_tops, row_totals = lax.map(forward_step, query_heads)
    attended_rows = attended.reshape(tokens, columns)
    own_rows = lax.dynamic_slice_in_dim(out_weight, head_index * columns, columns, 0)
    part_weight = own_rows
    summed_rows = lax.psum_scatter(
        lax.dot_general(
            part_weight, attended_rows, (((0,), (1,)), ((), ())), preferred_element_type=jnp.float32
        ).astype(jnp.bfloat16),
        "head",
        scatter_dimension=0,
        tiled=True,
    ).astype(jnp.float32)
    mixed_out = summed_rows.T.astype(jnp.bfloat16)
    part_weight = own_rows
    attended_grad = lax.dot_general(
        lax.all_gather(out_grad, "head", axis=1, tiled=True),
        part_weight,
        (((1,), (1,)), ((), ())),
        preferred_element_type=jnp.float32,
    )
    grad_heads = attended_grad.astype(jnp.bfloat16).reshape(
        block_total, query_block, heads_here, HEAD_DIM
    )

    def backward_step(totals, inputs):
        key_total, value_total = totals
        query_part, out_part, grad_part, row_top, row_total = inputs
        scores = score_rows(query_part, key_heads, score_scale)
        probability = jnp.exp(scores - row_top) / row_total
        weights = probability.astype(jnp.bfloat16)
        grad_prob = jnp.einsum(
            "qhd,khd->hqk", grad_part, value_heads, preferred_element_type=jnp.float32
        )
        row_delta = jnp.einsum(
            "qhd,qhd->hq", out_part, grad_part, preferred_element_type=jnp.float32
        )[:, :, None]
        grad_scores = (probability * (grad_prob - row_delta)).astype(jnp.bfloat16)
        query_part_grad = (
            jnp.einsum("hqk,khd->qhd", grad_scores, key_heads, preferred_element_type=jnp.float32)
            * score_scale
        )
        key_total = (
            key_total
            + jnp.einsum(
                "hqk,qhd->khd", grad_scores, query_part, preferred_element_type=jnp.float32
            )
            * score_scale
        )
        value_total = value_total + jnp.einsum(
            "hqk,qhd->khd", weights, grad_part, preferred_element_type=jnp.float32
        )
        return ((key_total, value_total), query_part_grad.astype(jnp.bfloat16))

    zero_keys = jnp.zeros((key_count, heads_here, HEAD_DIM), jnp.float32)
    (key_total, value_total), query_grads = lax.scan(
        backward_step,
        (zero_keys, zero_keys),
        (query_heads, attended, grad_heads, row_tops, row_totals),
    )
    query_grad = query_grads.reshape(tokens, columns)
    slot_grads = jnp.concatenate(
        [key_total.reshape(key_count, columns), value_total.reshape(key_count, columns)], axis=1
    )
    slot_grads = slot_grads.reshape(slot_count, BLOCK_TOKENS * 2 * columns)
    placing = (
        landing[None, :] == jnp.arange(peer_count * capacity, dtype=jnp.int32)[:, None]
    ).astype(jnp.float32)
    outgoing_grads = jnp.dot(placing, slot_grads, precision=lax.Precision.HIGHEST).reshape(
        peer_count, capacity, BLOCK_TOKENS, 2 * columns
    )
    returned = lax.all_to_all(
        outgoing_grads.astype(jnp.bfloat16), "view", split_axis=0, concat_axis=0, tiled=True
    ).astype(outgoing_grads.dtype)
    gathering = (
        chosen.reshape(-1)[None, :] == jnp.arange(block_count, dtype=jnp.int32)[:, None]
    ) & filled.reshape(-1)[None, :]
    summed = jnp.dot(
        gathering.astype(jnp.float32),
        returned.reshape(peer_count * capacity, BLOCK_TOKENS * 2 * columns),
        precision=lax.Precision.HIGHEST,
    )
    summed = summed.reshape(tokens, 2 * columns)
    key_grad = summed[:, :columns].astype(jnp.bfloat16)
    value_grad = summed[:, columns:].astype(jnp.bfloat16)
    return (mixed_out, query_grad, key_grad, value_grad)


def planes(*args):
    return plane_body(*args)


def solution(mesh):
    placed = P("view", "head")
    views, group = mesh.shape["view"], mesh.shape["head"]

    def step(*args):
        tokens, columns = args[0].shape
        count = columns // group // HEAD_DIM
        fits = (
            views == 2 * count
            and count > 1
            and count & (count - 1) == 0
            and group & (group - 1) == 0
            and tokens // views % (4 * BLOCK_TOKENS) == 0
        )
        inner = jax.shard_map(
            planes if fits else body,
            mesh=mesh,
            in_specs=(placed, placed, placed, P(), placed, P(), P()),
            out_specs=(placed,) * 4,
            check_vma=False,
        )
        return inner(*args)

    return step
```

```python
import jax
import jax.numpy as jnp
from jax import lax
from jax.experimental import pallas as pl
from jax.experimental.pallas import tpu as pltpu
from jax.sharding import PartitionSpec as P


HEAD_DIM = 64
BLOCK_TOKENS = 128
SCALE = HEAD_DIM**-0.5
LOG2E = 1.4426950408889634
F32 = jnp.float32
BF16 = jnp.bfloat16
HBM = pl.BlockSpec(memory_space=pl.ANY)
STEP = 256


def join(a, b):
    return jnp.concatenate([a[:, :HEAD_DIM], b[:, :HEAD_DIM]], axis=1)


def join_high(a, b):
    return jnp.concatenate([a[:, HEAD_DIM:], b[:, HEAD_DIM:]], axis=1)


def dot(a, b):
    return jnp.dot(a, b, preferred_element_type=F32)


def aligned(index, size):
    return pl.ds(pl.multiple_of(index * size, size), size)


def call(kernel, scalars, args, in_specs, out_specs, out_shape, grid=(1,), scratch=(), flops=0):
    return pl.pallas_call(
        kernel,
        grid_spec=pltpu.PrefetchScalarGridSpec(
            num_scalar_prefetch=len(scalars),
            grid=grid,
            in_specs=in_specs,
            out_specs=out_specs,
            scratch_shapes=list(scratch),
        ),
        out_shape=out_shape,
        compiler_params=pltpu.CompilerParams(dimension_semantics=("arbitrary",) * len(grid)),
        cost_estimate=pl.CostEstimate(flops=flops, transcendentals=0, bytes_accessed=0)
        if flops
        else None,
    )(*scalars, *args)


def whole(*shape):
    return pl.BlockSpec(shape, lambda *_: (0,) * len(shape))


def shape_of(*shape, dtype=BF16):
    return jax.ShapeDtypeStruct(shape, dtype)


def run_copies(*copies):
    for copy in copies:
        copy.start()
    for copy in copies:
        copy.wait()


def fold_pair(x_ref, out_ref):
    rows = out_ref.shape[2]
    top, low = x_ref[:rows, :], x_ref[rows:, :]
    for n in range(out_ref.shape[0]):
        out_ref[n, 0] = join(top, low)
        out_ref[n, 1] = join_high(top, low)


def fold_each(meta_ref, x_ref, outs):
    rows = x_ref.shape[0]
    count = x_ref.shape[1] // HEAD_DIM
    for n in range(count):
        head = meta_ref[0] ^ n
        pair = aligned(head // 2, 128)
        top, low = x_ref[: rows // 2, pair], x_ref[rows // 2 :, pair]
        folded = jnp.where(head % 2 == 1, join_high(top, low), join(top, low))
        for out in outs[n::count]:
            out[...] = folded


def pack_k(x_ref, out_ref):
    fold_pair(x_ref, out_ref)


def pack_v(meta_ref, x_ref, *outs):
    fold_each(meta_ref, x_ref, outs)


def pack_q(meta_ref, x_ref, *outs):
    fold_each(meta_ref, x_ref, outs)


def spread(parts, out_ref):
    rows = out_ref.shape[0] // 2
    for head in range(0, len(parts), 2):
        lanes = slice(HEAD_DIM * head, HEAD_DIM * (head + 2))
        out_ref[:rows, lanes] = join(parts[head], parts[head + 1])
        out_ref[rows:, lanes] = join_high(parts[head], parts[head + 1])


def collect(meta_ref, *refs):
    parts, (out_ref, scr, sem) = refs[:-3], refs[-3:]
    run_copies(
        *(
            pltpu.make_async_copy(part, scr.at[meta_ref[0] ^ n], sem.at[n])
            for n, part in enumerate(parts)
        )
    )
    spread([scr[n] for n in range(len(parts))], out_ref)


def total_pair(x_ref, out_ref):
    parts = []
    for head in range(2):
        part = x_ref[0, head].astype(F32)
        for n in range(1, x_ref.shape[0]):
            part = part + x_ref[n, head].astype(F32)
        parts.append(part.astype(BF16))
    spread(parts, out_ref)


def total_k(x_ref, out_ref):
    total_pair(x_ref, out_ref)


def total_v(x_ref, out_ref):
    total_pair(x_ref, out_ref)


def attended_grads(meta_ref, own_ref, *refs):
    count = own_ref.shape[1] // HEAD_DIM
    outs, scr = refs[-1 - count : -1], refs[-1]
    parts, w_ref = (own_ref, *refs[: -2 - count]), refs[-2 - count]
    columns = own_ref.shape[1]
    total = None
    for n, part in enumerate(parts):
        piece = lax.dot_general(
            part[...],
            w_ref[:, aligned(meta_ref[2] ^ n, columns)],
            (((1,), (1,)), ((), ())),
            preferred_element_type=F32,
        )
        total = piece if total is None else total + piece
    scr[...] = total.astype(BF16)
    fold_each(meta_ref, scr, outs)


def mix(meta_ref, *refs):
    parts, (w_ref, out_ref) = refs[:-2], refs[-2:]
    columns = out_ref.shape[1]
    total = None
    for n, part in enumerate(parts):
        piece = dot(part[...], w_ref[aligned(meta_ref[2] ^ n, columns), :])
        total = piece if total is None else total + piece
    out_ref[...] = total.astype(BF16)


def place(sv_ref, sb_ref, view, slot, per_half):
    block = sb_ref[view, slot]
    return sv_ref[view, slot], lax.div(block, per_half), aligned(lax.rem(block, per_half), BLOCK_TOKENS)


def gather(sv_ref, sb_ref, view, src, rows_scr=None, turned_scr=None):
    per_half = src.shape[1] // BLOCK_TOKENS
    for slot in range(sv_ref.shape[1]):
        source, high, rows = place(sv_ref, sb_ref, view, slot, per_half)
        block = src[source, rows, :]
        block = jnp.where(high == 1, join_high(block, block), block)
        span = slice(slot * BLOCK_TOKENS, (slot + 1) * BLOCK_TOKENS)
        if rows_scr is not None:
            rows_scr[span, :] = block
        if turned_scr is not None:
            turned_scr[:, span] = block.T[:HEAD_DIM]


def scatter(sv_ref, sb_ref, view, acc, lhs, rhs):
    per_view = acc.shape[1] // BLOCK_TOKENS
    keys = sv_ref.shape[1] * BLOCK_TOKENS
    for start in range(0, keys, STEP):
        part = None
        for a, b in zip(lhs, rhs):
            piece = dot(a[start : start + STEP, :], b)
            part = piece if part is None else part + piece
        for inner in range(0, STEP, BLOCK_TOKENS):
            source, _, rows = place(sv_ref, sb_ref, view, (start + inner) // BLOCK_TOKENS, per_view)
            acc[source, rows, :] += part[inner : inner + BLOCK_TOKENS]


def give_back(acc, out_ref):
    rows = out_ref.shape[1]
    for view in range(acc.shape[0]):
        block = acc[view].astype(BF16)
        out_ref[view] = join(block[:rows], block[rows:])


def halves(block):
    t = block.T
    return [t[:HEAD_DIM], t[HEAD_DIM:]]


def padded(t):
    return jnp.concatenate([t, jnp.zeros_like(t)], axis=0)


def view_copies(meta_ref, count, parts, scr, sems):
    here = meta_ref[1] * count + meta_ref[0]
    return [
        pltpu.make_async_copy(part, scr.at[here ^ n], sem)
        for n, (part, sem) in enumerate(zip(parts, sems))
    ]


def scores(sv_ref, sb_ref, meta_ref, k_ref, *refs):
    e_ref, l_ref, k_scr, q_scr, rows_scr, top_scr, s0, s1, sem = refs[-9:]
    parts = refs[:-9]
    count = len(parts)
    step = pl.program_id(0)
    keys, queries = s0.shape
    chunk = 128

    @pl.when(step == 0)
    def _():
        run_copies(
            pltpu.make_async_copy(k_ref, k_scr, sem.at[count]),
            *(pltpu.make_async_copy(p, q_scr.at[n], sem.at[n]) for n, p in enumerate(parts)),
        )

    def phase(old, new, q, n):
        top = None
        total = None
        old_top = top_scr[...]
        for i in range(0, keys, chunk):
            rows = slice(i, i + chunk)
            if q is not None:
                s = dot(rows_scr[rows, :], q)
                new[rows, :] = s
                m = jnp.max(s.reshape(chunk // 8, 8, queries), axis=0)
                top = m if top is None else jnp.maximum(top, m)
            e = jnp.exp2((old[rows, :] - old_top) * LOG2E)
            m = jnp.sum(e.reshape(chunk // 8, 8, queries), axis=0)
            total = m if total is None else total + m
            e_ref[0, n, rows, :] = e.astype(BF16)
        l_ref[0, n] = jnp.sum(total, axis=0, keepdims=True)
        if q is not None:
            top_scr[...] = jnp.max(top, axis=0, keepdims=True)

    @pl.when(step < count)
    def _():
        view = meta_ref[1] * count + (meta_ref[0] ^ step)
        gather(sv_ref, sb_ref, view, k_scr, rows_scr=rows_scr)
        first, second = [padded(t * jnp.asarray(SCALE, BF16)) for t in halves(q_scr[step])]
        phase(s1, s0, first, 0)
        phase(s0, s1, second, 1)

    @pl.when(step == count)
    def _():
        phase(s1, None, None, 0)


def attend(sv_ref, sb_ref, meta_ref, *refs):
    v_scr, g_scr, turned_scr, acc, sem = refs[-5:]
    count, views = g_scr.shape[0], v_scr.shape[0]
    v_parts, parts = refs[:views], refs[views : views + count]
    e_refs = refs[views + count : views + count + 2]
    l_refs = refs[views + count + 2 : views + count + 4]
    outs = refs[views + count + 4 : views + 2 * count + 4]
    delta_ref, dv_ref = refs[views + 2 * count + 4 : -5]
    step = pl.program_id(0)

    @pl.when(step == 0)
    def _():
        run_copies(
            *view_copies(meta_ref, count, v_parts, v_scr, [sem.at[count + n] for n in range(views)]),
            *(pltpu.make_async_copy(p, g_scr.at[n], sem.at[n]) for n, p in enumerate(parts)),
        )
        acc[...] = jnp.zeros_like(acc)

    view = meta_ref[1] * count + (meta_ref[0] ^ step)
    gather(sv_ref, sb_ref, view, v_scr, turned_scr=turned_scr)
    out, grads = [], []
    for n, g in enumerate(halves(g_scr[step])):
        l = l_refs[n][0, 0]
        o = (dot(turned_scr[...], e_refs[n][0, 0]) / l).astype(BF16)
        g = (g.astype(F32) / l).astype(BF16)
        delta_ref[0, n] = jnp.sum(o.astype(F32) * g.astype(F32), axis=0, keepdims=True)
        out.append(o)
        grads.append(padded(g).T)
    out = jnp.concatenate(out, axis=0).T
    for n, ref in enumerate(outs):

        @pl.when(step == n)
        def _():
            ref[...] = out

    scatter(sv_ref, sb_ref, view, acc, [e.at[0, 0] for e in e_refs], grads)

    @pl.when(step == count - 1)
    def _():
        give_back(acc, dv_ref)


def backward(sv_ref, sb_ref, meta_ref, k_ref, *refs):
    k_scr, v_scr, q_scr, g_scr, rows_scr, turned_scr, ds0, ds1, acc, sem = refs[-10:]
    count, views = q_scr.shape[0], v_scr.shape[0]
    v_parts, refs = refs[:views], refs[views:]
    q_parts, g_parts = refs[:count], refs[count : 2 * count]
    e_refs, l_refs = refs[2 * count : 2 * count + 2], refs[2 * count + 2 : 2 * count + 4]
    delta_ref = refs[2 * count + 4]
    outs = refs[2 * count + 5 : 3 * count + 5]
    dk_ref = refs[3 * count + 5]
    step = pl.program_id(0)

    @pl.when(step == 0)
    def _():
        run_copies(
            pltpu.make_async_copy(k_ref, k_scr, sem.at[2 * count]),
            *view_copies(
                meta_ref, count, v_parts, v_scr, [sem.at[2 * count + 1 + n] for n in range(views)]
            ),
            *(pltpu.make_async_copy(p, q_scr.at[n], sem.at[n]) for n, p in enumerate(q_parts)),
            *(
                pltpu.make_async_copy(p, g_scr.at[n], sem.at[count + n])
                for n, p in enumerate(g_parts)
            ),
        )
        acc[...] = jnp.zeros_like(acc)

    view = meta_ref[1] * count + (meta_ref[0] ^ step)
    gather(sv_ref, sb_ref, view, v_scr, rows_scr=rows_scr)
    gather(sv_ref, sb_ref, view, k_scr, turned_scr=turned_scr)
    keys = rows_scr.shape[0]
    queries = [padded(t * jnp.asarray(SCALE, BF16)).T for t in halves(q_scr[step])]
    for n, (g, ds_scr) in enumerate(zip(halves(g_scr[step]), (ds0, ds1))):
        g = padded((g.astype(F32) / l_refs[n][0, 0]).astype(BF16))
        for i in range(0, keys, STEP):
            dp = dot(rows_scr[i : i + STEP, :], g)
            e = e_refs[n][0, 0, i : i + STEP, :].astype(F32)
            ds_scr[i : i + STEP, :] = (e * (dp - delta_ref[0, n])).astype(BF16)
    scatter(sv_ref, sb_ref, view, acc, (ds0, ds1), queries)
    dq = [(dot(turned_scr[...], ds[...]) * SCALE).astype(BF16) for ds in (ds0, ds1)]
    dq = jnp.concatenate(dq, axis=0).T
    for n, ref in enumerate(outs):

        @pl.when(step == n)
        def _():
            ref[...] = dq

    @pl.when(step == count - 1)
    def _():
        give_back(acc, dk_ref)


def plane_body(query_rows, key_rows, value_rows, out_weight, out_grad, source_view, source_block):
    tokens, columns = query_rows.shape
    half = tokens // 2
    count = columns // HEAD_DIM
    views = lax.axis_size("view")
    group = lax.axis_size("head")
    keys = source_view.shape[1] * BLOCK_TOKENS
    head_index = lax.axis_index("head").astype(jnp.int32)
    view_index = lax.axis_index("view").astype(jnp.int32)
    meta = jnp.stack([lax.rem(view_index, count), lax.div(view_index, count), head_index])
    routes = (source_view, source_block, meta)

    def flip(x, bits):
        return lax.ppermute(x, "head", [(n, n ^ bits) for n in range(group)])

    def gathered(x):
        parts = {0: x}
        bits = group // 2
        while bits:
            for n, part in list(parts.items()):
                parts[n + bits] = flip(part, bits)
            bits //= 2
        return [parts[n] for n in range(group)]

    def view_swap(x):
        return lax.all_to_all(x, "view", split_axis=0, concat_axis=0, tiled=True)

    def send(parts):
        return [parts[0]] + [
            lax.ppermute(part, "view", [(n, n ^ bits) for n in range(views)])
            for bits, part in enumerate(parts)
            if bits
        ]

    full, rows_shape = whole(tokens, columns), shape_of(tokens, columns)
    one, one_shape = whole(half, 128), shape_of(half, 128)
    every, every_shape = whole(views, half, 128), shape_of(views, half, 128)
    groups = views // count
    strip = pl.BlockSpec((tokens, 128), lambda i: (0, i))
    duo = pl.BlockSpec((groups, 2, half, 128), lambda i: (0, i, 0, 0))
    duo_shape = shape_of(groups, count, half, 128)

    def packed(kernel, x):
        out = call(kernel, (), (x,), [strip], duo, duo_shape, grid=(count // 2,))
        return out.reshape(views, half, 128)

    def totalled(kernel, x):
        x = x.reshape(groups, count, half, 128)
        return call(kernel, (), (x,), [duo], strip, rows_shape, grid=(count // 2,))

    k = packed(pack_k, key_rows)
    k = view_swap(k)
    q = call(pack_q, (meta,), (query_rows,), [full], [one] * count, [one_shape] * count)
    q = send(q)
    og = gathered(out_grad)
    v = call(pack_v, (meta,), (value_rows,), [full], [one] * views, [one_shape] * views)
    v = send(v)
    g = call(
        attended_grads,
        (meta,),
        (*og, out_weight),
        [full] * group + [pl.BlockSpec((columns, group * columns), lambda i, m: (m[2], 0))],
        [one] * count,
        [one_shape] * count,
        scratch=[pltpu.VMEM((tokens, columns), BF16)],
    )
    g = send(g)
    e_spec = pl.BlockSpec((1, 2, keys, half), lambda i, *_: (i, 0, 0, 0))
    e_specs = [
        pl.BlockSpec((1, 1, keys, half), lambda i, *_: (i, 1, 0, 0)),
        pl.BlockSpec((1, 1, keys, half), lambda i, *_: (i + 1, 0, 0, 0)),
    ]
    l_specs = [
        pl.BlockSpec((1, 1, 1, half), lambda i, *_: (i, 1, 0, 0)),
        pl.BlockSpec((1, 1, 1, half), lambda i, *_: (i + 1, 0, 0, 0)),
    ]
    row_spec = pl.BlockSpec((1, 2, 1, half), lambda i, *_: (i, 0, 0, 0))
    row_shape = shape_of(count, 2, 1, half, dtype=F32)
    unit = 2 * count * keys * tokens * HEAD_DIM
    held = pltpu.VMEM((views, half, 128), BF16)
    mine = pltpu.VMEM((count, half, 128), BF16)
    totals = pltpu.VMEM((views, tokens, 128), F32)
    rows_scr = pltpu.VMEM((keys, 128), BF16)
    turned_scr = pltpu.VMEM((HEAD_DIM, keys), BF16)
    e, l = call(
        scores,
        routes,
        (k, *q),
        [HBM] * (1 + count),
        [e_spec, row_spec],
        [shape_of(count + 1, 2, keys, half), shape_of(count + 1, 2, 1, half, dtype=F32)],
        grid=(count + 1,),
        scratch=[
            held, mine, rows_scr, pltpu.VMEM((1, half), F32), pltpu.VMEM((keys, half), F32), pltpu.VMEM((keys, half), F32),
            pltpu.SemaphoreType.DMA((count + 1,)),
        ],
        flops=unit * 4,
    )
    *o, delta, dv = call(
        attend,
        routes,
        (*v, *g, e, e, l, l),
        [HBM] * (views + count) + e_specs + l_specs,
        [one] * count + [row_spec, every],
        [one_shape] * count + [row_shape, every_shape],
        grid=(count,),
        scratch=[held, mine, turned_scr, totals, pltpu.SemaphoreType.DMA((count + views,))],
        flops=unit * 3,
    )
    dv = view_swap(dv)
    o = send(o)
    *dq, dk = call(
        backward,
        routes,
        (k, *v, *q, *g, e, e, l, l, delta),
        [HBM] * (1 + views + 2 * count) + e_specs + l_specs + [row_spec],
        [one] * count + [every],
        [one_shape] * count + [every_shape],
        grid=(count,),
        scratch=[
            held, held, mine, mine, rows_scr, turned_scr,
            pltpu.VMEM((keys, half), BF16), pltpu.VMEM((keys, half), BF16),
            totals, pltpu.SemaphoreType.DMA((2 * count + 1 + views,)),
        ],
        flops=unit * 8,
    )
    dk = view_swap(dk)
    dq = send(dq)

    def collected(parts):
        return call(
            collect, (meta,), tuple(parts), [HBM] * count, full, rows_shape,
            scratch=[mine, pltpu.SemaphoreType.DMA((count,))],
        )

    attended = collected(o)
    attended = gathered(attended)
    mixed_out = call(
        mix,
        (meta,),
        (*attended, out_weight),
        [full] * group + [pl.BlockSpec((group * columns, columns), lambda i, m: (0, m[2]))],
        full,
        rows_shape,
    )
    value_grad = totalled(total_v, dv)
    query_grad = collected(dq)
    key_grad = totalled(total_k, dk)
    return mixed_out, query_grad, key_grad, value_grad


def score_rows(query_part, key_heads, score_scale):
    return (
        jnp.einsum("qhd,khd->hqk", query_part, key_heads, preferred_element_type=jnp.float32)
        * score_scale
    )


def body(query_rows, key_rows, value_rows, out_weight, out_grad, source_view, source_block):
    tokens = query_rows.shape[0]
    columns = query_rows.shape[1]
    heads_here = columns // HEAD_DIM
    slot_count = source_view.shape[1]
    key_count = slot_count * BLOCK_TOKENS
    peer_count = lax.axis_size("view")
    capacity = max(1, 2 * slot_count // peer_count)
    block_count = tokens // BLOCK_TOKENS
    view_index = lax.axis_index("view")
    head_index = lax.axis_index("head")
    score_scale = HEAD_DIM ** (-0.5)
    slot_order = jnp.arange(slot_count, dtype=jnp.int32)
    same_view = source_view[:, :, None] == source_view[:, None, :]
    earlier = slot_order[None, :] < slot_order[:, None]
    slot_rank = jnp.sum((same_view & earlier[None]).astype(jnp.int32), axis=2)
    copy_order = jnp.arange(capacity, dtype=jnp.int32)
    matched = (source_view == view_index)[:, :, None] & (
        slot_rank[:, :, None] == copy_order[None, None, :]
    )
    filled = jnp.any(matched, axis=1)
    chosen = jnp.sum(jnp.where(matched, source_block[:, :, None], 0), axis=1)
    own_view = lax.dynamic_index_in_dim(source_view, view_index, 0, keepdims=False)
    own_rank = lax.dynamic_index_in_dim(slot_rank, view_index, 0, keepdims=False)
    landing = own_view * capacity + own_rank
    joined = jnp.concatenate([key_rows, value_rows], axis=1)
    outgoing = jnp.take(
        joined.reshape(block_count, BLOCK_TOKENS, 2 * columns), chosen.reshape(-1), axis=0
    )
    outgoing = outgoing.reshape(peer_count, capacity, BLOCK_TOKENS, 2 * columns)
    incoming = lax.all_to_all(outgoing, "view", split_axis=0, concat_axis=0, tiled=True)
    fetched = jnp.take(
        incoming.reshape(peer_count * capacity, BLOCK_TOKENS, 2 * columns), landing, axis=0
    )
    fetched = fetched.reshape(key_count, 2 * columns)
    query_block = min(512, tokens)
    block_total = tokens // query_block
    key_heads = fetched[:, :columns].reshape(key_count, heads_here, HEAD_DIM)
    value_heads = fetched[:, columns:].reshape(key_count, heads_here, HEAD_DIM)
    query_heads = query_rows.reshape(block_total, query_block, heads_here, HEAD_DIM)

    def forward_step(query_part):
        scores = score_rows(query_part, key_heads, score_scale)
        row_top = jnp.max(scores, axis=-1, keepdims=True)
        shifted = jnp.exp(scores - row_top)
        row_total = jnp.sum(shifted, axis=-1, keepdims=True)
        weights = (shifted / row_total).astype(jnp.bfloat16)
        out_part = jnp.einsum(
            "hqk,khd->qhd", weights, value_heads, preferred_element_type=jnp.float32
        )
        return (out_part.astype(jnp.bfloat16), row_top, row_total)

    attended, row_tops, row_totals = lax.map(forward_step, query_heads)
    attended_rows = attended.reshape(tokens, columns)
    own_rows = lax.dynamic_slice_in_dim(out_weight, head_index * columns, columns, 0)
    part_weight = own_rows
    summed_rows = lax.psum_scatter(
        lax.dot_general(
            part_weight, attended_rows, (((0,), (1,)), ((), ())), preferred_element_type=jnp.float32
        ).astype(jnp.bfloat16),
        "head",
        scatter_dimension=0,
        tiled=True,
    ).astype(jnp.float32)
    mixed_out = summed_rows.T.astype(jnp.bfloat16)
    part_weight = own_rows
    attended_grad = lax.dot_general(
        lax.all_gather(out_grad, "head", axis=1, tiled=True),
        part_weight,
        (((1,), (1,)), ((), ())),
        preferred_element_type=jnp.float32,
    )
    grad_heads = attended_grad.astype(jnp.bfloat16).reshape(
        block_total, query_block, heads_here, HEAD_DIM
    )

    def backward_step(totals, inputs):
        key_total, value_total = totals
        query_part, out_part, grad_part, row_top, row_total = inputs
        scores = score_rows(query_part, key_heads, score_scale)
        probability = jnp.exp(scores - row_top) / row_total
        weights = probability.astype(jnp.bfloat16)
        grad_prob = jnp.einsum(
            "qhd,khd->hqk", grad_part, value_heads, preferred_element_type=jnp.float32
        )
        row_delta = jnp.einsum(
            "qhd,qhd->hq", out_part, grad_part, preferred_element_type=jnp.float32
        )[:, :, None]
        grad_scores = (probability * (grad_prob - row_delta)).astype(jnp.bfloat16)
        query_part_grad = (
            jnp.einsum("hqk,khd->qhd", grad_scores, key_heads, preferred_element_type=jnp.float32)
            * score_scale
        )
        key_total = (
            key_total
            + jnp.einsum(
                "hqk,qhd->khd", grad_scores, query_part, preferred_element_type=jnp.float32
            )
            * score_scale
        )
        value_total = value_total + jnp.einsum(
            "hqk,qhd->khd", weights, grad_part, preferred_element_type=jnp.float32
        )
        return ((key_total, value_total), query_part_grad.astype(jnp.bfloat16))

    zero_keys = jnp.zeros((key_count, heads_here, HEAD_DIM), jnp.float32)
    (key_total, value_total), query_grads = lax.scan(
        backward_step,
        (zero_keys, zero_keys),
        (query_heads, attended, grad_heads, row_tops, row_totals),
    )
    query_grad = query_grads.reshape(tokens, columns)
    slot_grads = jnp.concatenate(
        [key_total.reshape(key_count, columns), value_total.reshape(key_count, columns)], axis=1
    )
    slot_grads = slot_grads.reshape(slot_count, BLOCK_TOKENS * 2 * columns)
    placing = (
        landing[None, :] == jnp.arange(peer_count * capacity, dtype=jnp.int32)[:, None]
    ).astype(jnp.float32)
    outgoing_grads = jnp.dot(placing, slot_grads, precision=lax.Precision.HIGHEST).reshape(
        peer_count, capacity, BLOCK_TOKENS, 2 * columns
    )
    returned = lax.all_to_all(
        outgoing_grads.astype(jnp.bfloat16), "view", split_axis=0, concat_axis=0, tiled=True
    ).astype(outgoing_grads.dtype)
    gathering = (
        chosen.reshape(-1)[None, :] == jnp.arange(block_count, dtype=jnp.int32)[:, None]
    ) & filled.reshape(-1)[None, :]
    summed = jnp.dot(
        gathering.astype(jnp.float32),
        returned.reshape(peer_count * capacity, BLOCK_TOKENS * 2 * columns),
        precision=lax.Precision.HIGHEST,
    )
    summed = summed.reshape(tokens, 2 * columns)
    key_grad = summed[:, :columns].astype(jnp.bfloat16)
    value_grad = summed[:, columns:].astype(jnp.bfloat16)
    return (mixed_out, query_grad, key_grad, value_grad)


def planes(*args):
    return plane_body(*args)


def solution(mesh):
    placed = P("view", "head")
    views, group = mesh.shape["view"], mesh.shape["head"]

    def step(*args):
        tokens, columns = args[0].shape
        count = columns // group // HEAD_DIM
        fits = (
            views == 2 * count
            and count > 1
            and count & (count - 1) == 0
            and group & (group - 1) == 0
            and tokens // views % (4 * BLOCK_TOKENS) == 0
        )
        inner = jax.shard_map(
            planes if fits else body,
            mesh=mesh,
            in_specs=(placed, placed, placed, P(), placed, P(), P()),
            out_specs=(placed,) * 4,
            check_vma=False,
        )
        return inner(*args)

    return step
```
